16 devices in a mesh: tp: 4 (over z, y), cp: 4 (over x, core).
Axes of the slice: x: 2, y: 2, z: 2, core: 2. Of those that a mesh axis runs over, the one named last changes fastest.
Arguments:
- query_in: bfloat16 [32, 32, 48, 128], P(None, 'cp', 'tp'), parts along dimension 2
- attn_out: bfloat16 [32, 32, 48, 128], P(None, 'cp', 'tp'), parts along dimension 2
- grad_out: bfloat16 [32, 32, 48, 128], P(None, 'cp', 'tp'), parts along dimension 2
- log_sum: float32 [32, 32, 48], P(None, 'cp', 'tp'), parts along dimension 2
- key_cache: bfloat16 [9216, 8, 128], P('cp', 'tp'), parts along dimension 1
- value_cache: bfloat16 [9216, 8, 128], P('cp', 'tp'), parts along dimension 1
Outputs:
- output 1: bfloat16 [32, 32, 48, 128], P(None, 'cp', 'tp'), parts along dimension 2
- output 2: float32 [9216, 8, 128], P('cp', 'tp'), parts along dimension 1
- output 3: float32 [9216, 8, 128], P('cp', 'tp'), parts along dimension 1
There are 4 independent parts. The reference program is written for one: setup_inputs(seed, part) draws one part's arguments, and reference() takes and returns one part's arrays. A program takes and returns all parts, laid end to end along the dimension named above; each array names one.
All inputs are finite; a program needn't handle non-finite values.
Results may differ from the reference program's by a relative error of at most 0.001.
Values are sent between devices in bfloat16 or wider.
A program may use at most 1 GiB of HBM per device.

```python
import math
import jax
import jax.numpy as jnp
from jax import lax

SLICE_COUNT = 32
SLICE_LEN = 32
PREFIX = 8192
Q_HEADS = 12
KV_HEADS = 2
HEAD_DIM = 128

TOTAL_LEN = PREFIX + SLICE_COUNT * SLICE_LEN
GROUP_SIZE = Q_HEADS // KV_HEADS
QUERY_ROWS = SLICE_COUNT * SLICE_LEN
BLOCK_ROWS = min(SLICE_LEN, 2 ** int(math.log2(max(1, 2 ** 24 // (Q_HEADS * TOTAL_LEN)))))
BLOCK_COUNT = QUERY_ROWS // BLOCK_ROWS
SOFTMAX_SCALE = HEAD_DIM ** -0.5
GRAD_SCALE = math.sqrt(TOTAL_LEN) / 8.0


def forward_stats(query_f, key_f, value_f):
    q_blocks = query_f.reshape(BLOCK_COUNT, BLOCK_ROWS, KV_HEADS, GROUP_SIZE, HEAD_DIM)
    key_pos = jnp.arange(TOTAL_LEN)

    def one_block(block_in):
        q_block, block_idx = block_in
        q_pos = PREFIX + block_idx * BLOCK_ROWS + jnp.arange(BLOCK_ROWS)
        causal = key_pos[None, :] <= q_pos[:, None]
        logits = jnp.einsum('qhgd,khd->hgqk', q_block, key_f) * SOFTMAX_SCALE
        logits = jnp.where(causal, logits, -jnp.inf)
        row_max = jnp.max(logits, axis=-1, keepdims=True)
        weights = jnp.exp(logits - row_max)
        row_sum = jnp.sum(weights, axis=-1, keepdims=True)
        out_block = jnp.einsum('hgqk,khd->qhgd', weights / row_sum, value_f)
        lse_block = jnp.transpose((row_max + jnp.log(row_sum))[..., 0], (2, 0, 1))
        return out_block.reshape(BLOCK_ROWS, Q_HEADS, HEAD_DIM), lse_block.reshape(BLOCK_ROWS, Q_HEADS)

    out_all, lse_all = lax.map(one_block, (q_blocks, jnp.arange(BLOCK_COUNT)))
    return out_all.reshape(QUERY_ROWS, Q_HEADS, HEAD_DIM), lse_all.reshape(QUERY_ROWS, Q_HEADS)


def setup_inputs(seed: int = 0, part: int = 0) -> dict:
    base_key = jax.random.fold_in(jax.random.key(seed), part)
    key_q, key_k, key_v, key_mean, key_grad = jax.random.split(base_key, 5)
    query_in = (1.2 * jax.random.normal(key_q, (QUERY_ROWS, Q_HEADS, HEAD_DIM), jnp.float32)).astype(jnp.bfloat16)
    key_cache = jax.random.normal(key_k, (TOTAL_LEN, KV_HEADS, HEAD_DIM), jnp.float32).astype(jnp.bfloat16)
    head_mean = 0.7 * jax.random.normal(key_mean, (1, KV_HEADS, HEAD_DIM), jnp.float32)
    value_cache = (head_mean + jax.random.normal(key_v, (TOTAL_LEN, KV_HEADS, HEAD_DIM), jnp.float32)).astype(jnp.bfloat16)
    out_f, lse_f = forward_stats(query_in.astype(jnp.float32), key_cache.astype(jnp.float32), value_cache.astype(jnp.float32))
    grad_noise = jax.random.normal(key_grad, (QUERY_ROWS, Q_HEADS, HEAD_DIM), jnp.float32)
    grad_out = (GRAD_SCALE * (0.5 * out_f + grad_noise)).astype(jnp.bfloat16)
    row_shape = (SLICE_COUNT, SLICE_LEN, Q_HEADS, HEAD_DIM)
    return {
        'query_in': query_in.reshape(row_shape),
        'attn_out': out_f.astype(jnp.bfloat16).reshape(row_shape),
        'grad_out': grad_out.reshape(row_shape),
        'log_sum': lse_f.reshape(SLICE_COUNT, SLICE_LEN, Q_HEADS),
        'key_cache': key_cache,
        'value_cache': value_cache,
    }


def reference(query_in, attn_out, grad_out, log_sum, key_cache, value_cache):
    key_f = key_cache.astype(jnp.float32)
    value_f = value_cache.astype(jnp.float32)
    block_shape = (BLOCK_COUNT, BLOCK_ROWS, KV_HEADS, GROUP_SIZE, HEAD_DIM)
    q_blocks = query_in.astype(jnp.float32).reshape(block_shape)
    o_blocks = attn_out.astype(jnp.float32).reshape(block_shape)
    g_blocks = grad_out.astype(jnp.float32).reshape(block_shape)
    l_blocks = log_sum.reshape(BLOCK_COUNT, BLOCK_ROWS, KV_HEADS, GROUP_SIZE)
    key_pos = jnp.arange(TOTAL_LEN)

    def block_step(acc_pair, block_in):
        grad_key, grad_value = acc_pair
        q_block, o_block, g_block, l_block, block_idx = block_in
        q_pos = PREFIX + block_idx * BLOCK_ROWS + jnp.arange(BLOCK_ROWS)
        causal = key_pos[None, :] <= q_pos[:, None]
        row_delta = jnp.transpose(jnp.sum(g_block * o_block, axis=-1), (1, 2, 0))[..., None]
        row_lse = jnp.transpose(l_block, (1, 2, 0))[..., None]
        logits = jnp.einsum('qhgd,khd->hgqk', q_block, key_f) * SOFTMAX_SCALE
        prob_f = jnp.where(causal, jnp.exp(logits - row_lse), 0.0)
        prob_b = prob_f.astype(jnp.bfloat16).astype(jnp.float32)
        grad_value = grad_value + jnp.einsum('hgqk,qhgd->khd', prob_b, g_block)
        grad_prob = jnp.einsum('qhgd,khd->hgqk', g_block, value_f)
        grad_score = (prob_f * (grad_prob - row_delta)).astype(jnp.bfloat16).astype(jnp.float32)
        grad_key = grad_key + jnp.einsum('hgqk,qhgd->khd', grad_score, q_block) * SOFTMAX_SCALE
        grad_q = jnp.einsum('hgqk,khd->qhgd', grad_score, key_f) * SOFTMAX_SCALE
        return (grad_key, grad_value), grad_q.astype(jnp.bfloat16)

    zero_acc = jnp.zeros((TOTAL_LEN, KV_HEADS, HEAD_DIM), jnp.float32)
    (grad_key, grad_value), grad_query = lax.scan(block_step, (zero_acc, zero_acc), (q_blocks, o_blocks, g_blocks, l_blocks, jnp.arange(BLOCK_COUNT)))
    return grad_query.reshape(SLICE_COUNT, SLICE_LEN, Q_HEADS, HEAD_DIM), grad_key, grad_value
```

```python
import jax
import jax.numpy as jnp
from jax import lax
from jax.experimental import pallas as pl
from jax.experimental.pallas import tpu as pltpu
from jax.sharding import PartitionSpec as P

MESH = pl.DeviceIdType.MESH
LOG2E = 1.4426950408889634
NT = (((1,), (1,)), ((), ()))
NN = (((1,), (0,)), ((), ()))
KEY_BLOCK = 256
OWN, PEER, ACROSS, DIAG = 0, 1, 2, 3
STEPS = [(0, 0), (1, 0), (0, 1), (2, 0), (3, 0), (1, 1), (2, 1), (3, 1), (0, 2), (2, 2), (3, 2), (1, 2), (2, 3), (3, 3), (0, 3), (1, 3)]
REDUCE_AT = [5, 8, 11, 14]


def dot(a, b, dims=NN):
    return lax.dot_general(a, b, dims, preferred_element_type=jnp.float32)


def table(step, values):
    out = jnp.int32(values[0])
    for i, v in enumerate(values[1:], 1):
        out = jnp.where(step == i, jnp.int32(v), out)
    return out


def make_kernel(n_slices, rows8, group, head_dim, key_rows, cp_size):
    half_slices = n_slices // 2
    unit = rows8 * group
    rows = half_slices * unit
    slice_len = rows8 * cp_size
    prefix = key_rows * cp_size - n_slices * slice_len
    n_blocks = key_rows // KEY_BLOCK
    scale = head_dim ** -0.5
    exp_scale = scale * LOG2E
    first_masked = max(0, prefix - (cp_size - 1) * key_rows) // KEY_BLOCK

    def kernel(q_hbm, o_hbm, g_hbm, l_hbm, k_hbm, v_hbm, dq_hbm, dk_hbm, dv_hbm,
               q_all, g_all, stat_all, o_own, lse_own, k_all, v_all, dk_t, dv_t, dq_all,
               from_peer_own, from_peer_across, from_across, q_t, g_t, p_a, s_a, p_b, s_b,
               lse_rep, del_rep, row_pos, dq_out, dk_out, dv_out,
               load_sem, q_recv, g_recv, stat_recv, q_send, g_send, stat_send,
               part_recv, part_send, store_sem):
        me = lax.axis_index('cp')
        chip, core = me // 2, me % 2
        peer = chip * 2 + (1 - core)
        across = (1 - chip) * 2 + core
        diag = (1 - chip) * 2 + (1 - core)

        barrier = pltpu.get_barrier_semaphore()
        for other in (peer, across):
            pl.semaphore_signal(barrier, inc=1, device_id={'cp': other}, device_id_type=MESH)

        def part(ref, ch):
            return ref.at[pl.ds((ch % 2) * half_slices, half_slices), ch // 2]

        loads = []
        for ch in range(4):
            loads.append(pltpu.make_async_copy(part(g_hbm, ch), g_all.at[OWN, ch], load_sem.at[ch]))
        for ch in range(4):
            loads.append(pltpu.make_async_copy(part(o_hbm, ch), o_own.at[ch], load_sem.at[4 + ch]))
        loads.append(pltpu.make_async_copy(l_hbm, lse_own, load_sem.at[8]))
        for ch in range(4):
            loads.append(pltpu.make_async_copy(part(q_hbm, ch), q_all.at[OWN, ch], load_sem.at[9 + ch]))
        loads.append(pltpu.make_async_copy(k_hbm, k_all, load_sem.at[13]))
        loads.append(pltpu.make_async_copy(v_hbm, v_all, load_sem.at[14]))
        for copy in loads:
            copy.start()

        def send_rows(ch, slot, other):
            q = pltpu.make_async_remote_copy(part(q_hbm, ch), q_all.at[slot, ch], q_send.at[slot, ch], q_recv.at[slot, ch], device_id={'cp': other}, device_id_type=MESH)
            g = pltpu.make_async_remote_copy(part(g_hbm, ch), g_all.at[slot, ch], g_send.at[slot, ch], g_recv.at[slot, ch], device_id={'cp': other}, device_id_type=MESH)
            return q, g

        def send_stat(src_slot, dst_slot, other):
            return pltpu.make_async_remote_copy(stat_all.at[src_slot], stat_all.at[dst_slot], stat_send.at[dst_slot], stat_recv.at[dst_slot], device_id={'cp': other}, device_id_type=MESH)

        def forward_rows(ch):
            q = pltpu.make_async_remote_copy(q_all.at[ACROSS, ch], q_all.at[DIAG, ch], q_send.at[DIAG, ch], q_recv.at[DIAG, ch], device_id={'cp': peer}, device_id_type=MESH)
            g = pltpu.make_async_remote_copy(g_all.at[ACROSS, ch], g_all.at[DIAG, ch], g_send.at[DIAG, ch], g_recv.at[DIAG, ch], device_id={'cp': peer}, device_id_type=MESH)
            return q, g

        def send_own_part(ch):
            return pltpu.make_async_remote_copy(dq_all.at[PEER, ch], from_peer_own.at[ch], part_send.at[0, ch], part_recv.at[0, ch], device_id={'cp': peer}, device_id_type=MESH)

        def send_diag_part(ch):
            return pltpu.make_async_remote_copy(dq_all.at[DIAG, ch], from_peer_across.at[ch], part_send.at[1, ch], part_recv.at[1, ch], device_id={'cp': peer}, device_id_type=MESH)

        def send_reduced(ch):
            return pltpu.make_async_remote_copy(dq_all.at[ACROSS, ch], from_across.at[ch], part_send.at[2, ch], part_recv.at[2, ch], device_id={'cp': across}, device_id_type=MESH)

        pl.semaphore_wait(barrier, 2)
        for slot, other in ((ACROSS, across), (PEER, peer)):
            for copy in send_rows(0, slot, other):
                copy.start()

        for copy in loads[:9]:
            copy.wait()
        lane = lax.broadcasted_iota(jnp.int32, (unit, 128), 1)
        for kv in range(2):
            acc = jnp.zeros((unit, 128), jnp.float32)
            for s in range(n_slices):
                ch = kv * 2 + s // half_slices
                prod = g_all[OWN, ch, s % half_slices].astype(jnp.float32) * o_own[ch, s % half_slices].astype(jnp.float32)
                acc = jnp.where(lane == n_slices + s, jnp.sum(prod, axis=1, keepdims=True), acc)
            stat_all[OWN, pl.ds(kv * group, group)] = acc.reshape(group, rows8, 128)
        stat_all[OWN, :, :, pl.ds(0, n_slices)] = lse_own[...] * LOG2E
        for slot, other in ((ACROSS, across), (PEER, peer)):
            send_stat(OWN, slot, other).start()
        for ch in range(1, 4):
            for slot, other in ((ACROSS, across), (PEER, peer)):
                for copy in send_rows(ch, slot, other):
                    copy.start()

        dk_t[...] = jnp.zeros_like(dk_t)
        dv_t[...] = jnp.zeros_like(dv_t)
        token = lax.broadcasted_iota(jnp.int32, (rows8, 128), 0)
        for s in range(half_slices):
            for h in range(group):
                row_pos[pl.ds((s * group + h) * rows8, rows8)] = token + s * slice_len
        for copy in loads[9:]:
            copy.wait()

        def step_body(step, carry):
            slot = table(step, [a for a, _ in STEPS])
            ch = table(step, [b for _, b in STEPS])
            kv, half = ch // 2, ch % 2
            source = jnp.where(slot == OWN, me, jnp.where(slot == PEER, peer, jnp.where(slot == ACROSS, across, diag)))

            @pl.when(slot != OWN)
            def _():
                pltpu.make_async_remote_copy(q_all.at[slot, ch], q_all.at[slot, ch], q_send.at[slot, ch], q_recv.at[slot, ch], device_id={'cp': peer}, device_id_type=MESH).wait_recv()
                pltpu.make_async_remote_copy(g_all.at[slot, ch], g_all.at[slot, ch], g_send.at[slot, ch], g_recv.at[slot, ch], device_id={'cp': peer}, device_id_type=MESH).wait_recv()

            @pl.when(jnp.logical_and(slot != OWN, ch == 0))
            def _():
                pltpu.make_async_remote_copy(stat_all.at[slot], stat_all.at[slot], stat_send.at[slot], stat_recv.at[slot], device_id={'cp': peer}, device_id_type=MESH).wait_recv()

            @pl.when(slot == ACROSS)
            def _():
                for copy in forward_rows(ch):
                    copy.start()

            @pl.when(jnp.logical_and(slot == ACROSS, ch == 0))
            def _():
                send_stat(ACROSS, DIAG, peer).start()

            q_t[...] = q_all[slot, ch].reshape(rows, head_dim).T
            g_t[...] = g_all[slot, ch].reshape(rows, head_dim).T
            for h in range(group):
                st = stat_all[slot, kv * group + h]
                st = jnp.where(half == 1, pltpu.roll(st, 128 - half_slices, 1), st)
                for s in range(half_slices):
                    at = pl.ds((s * group + h) * rows8, rows8)
                    lse_rep[at] = jnp.broadcast_to(st[:, s:s + 1], (rows8, 128))
                    del_rep[at] = jnp.broadcast_to(st[:, n_slices + s:n_slices + s + 1], (rows8, 128))

            def scores(block, p_buf, s_buf):
                keys = pl.ds(block * KEY_BLOCK, KEY_BLOCK)
                logits = dot(q_all[slot, ch].reshape(rows, head_dim), k_all[kv, keys], NT)
                lse = lse_rep[...]
                prob = jnp.exp2(logits * exp_scale - jnp.concatenate([lse, lse], 1))
                if block >= first_masked:
                    first = me * key_rows + block * KEY_BLOCK - prefix - half * (half_slices * slice_len) - source * rows8
                    key_pos = lax.broadcasted_iota(jnp.int32, (rows, KEY_BLOCK), 1) + first
                    pos = row_pos[...]
                    prob = jnp.where(key_pos <= jnp.concatenate([pos, pos], 1), prob, 0.0)
                grad_prob = dot(g_all[slot, ch].reshape(rows, head_dim), v_all[kv, keys], NT)
                delta = del_rep[...]
                p_buf[...] = prob.astype(jnp.bfloat16)
                s_buf[...] = (prob * (grad_prob - jnp.concatenate([delta, delta], 1))).astype(jnp.bfloat16)

            def grads(block, p_buf, s_buf):
                keys = pl.ds(block * KEY_BLOCK, KEY_BLOCK)
                dv_t[kv, :, keys] += dot(g_t[...], p_buf[...])
                dk_t[kv, :, keys] += dot(q_t[...], s_buf[...])
                part_q = dot(s_buf[...], k_all[kv, keys])
                if block == 0:
                    dq_all[slot, ch] = part_q
                else:
                    dq_all[slot, ch] += part_q

            bufs = ((p_a, s_a), (p_b, s_b))
            scores(0, *bufs[0])
            for block in range(n_blocks):
                if block + 1 < n_blocks:
                    scores(block + 1, *bufs[(block + 1) % 2])
                grads(block, *bufs[block % 2])

            @pl.when(slot == PEER)
            def _():
                send_own_part(ch).start()

            @pl.when(slot == DIAG)
            def _():
                send_diag_part(ch).start()

            reduce_ch = table(step, [REDUCE_AT.index(i) if i in REDUCE_AT else -1 for i in range(len(STEPS))])

            @pl.when(reduce_ch >= 0)
            def _():
                send_diag_part(reduce_ch).wait_recv()
                dq_all[ACROSS, reduce_ch] += from_peer_across[reduce_ch]
                send_reduced(reduce_ch).start()

            return carry

        lax.fori_loop(0, len(STEPS), step_body, 0)

        stores = []
        for i, (acc_t, out, hbm) in enumerate(((dv_t, dv_out, dv_hbm), (dk_t, dk_out, dk_hbm))):
            for block in range(n_blocks):
                keys = pl.ds(block * KEY_BLOCK, KEY_BLOCK)
                for kv in range(2):
                    grad = acc_t[kv, :, keys].T
                    if acc_t is dk_t:
                        grad = grad * scale
                    out[pl.ds(2 * block * KEY_BLOCK + kv, KEY_BLOCK, stride=2)] = grad
            stores.append(pltpu.make_async_copy(out, hbm, store_sem.at[i]))
            stores[-1].start()
        for ch in range(4):
            send_own_part(ch).wait_recv()
            send_reduced(ch).wait_recv()
            total = (dq_all[OWN, ch] + from_peer_own[ch] + from_across[ch]) * scale
            dq_out[ch] = total.astype(jnp.bfloat16).reshape(half_slices, unit, head_dim)
            stores.append(pltpu.make_async_copy(dq_out.at[ch], part(dq_hbm, ch), store_sem.at[2 + ch]))
            stores[-1].start()
        for copy in stores:
            copy.wait()
        for slot, other in ((ACROSS, across), (PEER, peer)):
            send_stat(OWN, slot, other).wait_send()
            for ch in range(4):
                for copy in send_rows(ch, slot, other):
                    copy.wait_send()
        send_stat(ACROSS, DIAG, peer).wait_send()
        for ch in range(4):
            for copy in forward_rows(ch):
                copy.wait_send()
            send_own_part(ch).wait_send()
            send_diag_part(ch).wait_send()
            send_reduced(ch).wait_send()

    bf16, f32 = jnp.bfloat16, jnp.float32
    chunk = (half_slices, unit, head_dim)
    scratch = [
        pltpu.VMEM((4, 4) + chunk, bf16),
        pltpu.VMEM((4, 4) + chunk, bf16),
        pltpu.VMEM((4, 2 * group, rows8, 128), f32),
        pltpu.VMEM((4,) + chunk, bf16),
        pltpu.VMEM((2 * group, rows8, n_slices), f32),
        pltpu.VMEM((2, key_rows, head_dim), bf16),
        pltpu.VMEM((2, key_rows, head_dim), bf16),
        pltpu.VMEM((2, head_dim, key_rows), f32),
        pltpu.VMEM((2, head_dim, key_rows), f32),
        pltpu.VMEM((4, 4, rows, head_dim), f32),
        pltpu.VMEM((4, rows, head_dim), f32),
        pltpu.VMEM((4, rows, head_dim), f32),
        pltpu.VMEM((4, rows, head_dim), f32),
        pltpu.VMEM((head_dim, rows), bf16),
        pltpu.VMEM((head_dim, rows), bf16),
        pltpu.VMEM((rows, KEY_BLOCK), bf16),
        pltpu.VMEM((rows, KEY_BLOCK), bf16),
        pltpu.VMEM((rows, KEY_BLOCK), bf16),
        pltpu.VMEM((rows, KEY_BLOCK), bf16),
        pltpu.VMEM((rows, 128), f32),
        pltpu.VMEM((rows, 128), f32),
        pltpu.VMEM((rows, 128), jnp.int32),
        pltpu.VMEM((4,) + chunk, bf16),
        pltpu.VMEM((2 * key_rows, head_dim), f32),
        pltpu.VMEM((2 * key_rows, head_dim), f32),
        pltpu.SemaphoreType.DMA((15,)),
        pltpu.SemaphoreType.DMA((4, 4)),
        pltpu.SemaphoreType.DMA((4, 4)),
        pltpu.SemaphoreType.DMA((4,)),
        pltpu.SemaphoreType.DMA((4, 4)),
        pltpu.SemaphoreType.DMA((4, 4)),
        pltpu.SemaphoreType.DMA((4,)),
        pltpu.SemaphoreType.DMA((3, 4)),
        pltpu.SemaphoreType.DMA((3, 4)),
        pltpu.SemaphoreType.DMA((6,)),
    ]
    return kernel, scratch


def solution(mesh):
    cp_size = mesh.shape['cp']
    row_spec = P(None, 'cp', 'tp', None)
    lse_spec = P(None, 'cp', 'tp')
    kv_spec = P('cp', 'tp', None)

    def local_backward(query_in, attn_out, grad_out, log_sum, key_cache, value_cache):
        n_slices, rows8, q_heads, head_dim = query_in.shape
        key_rows, kv_heads, _ = key_cache.shape
        group = q_heads // kv_heads
        kernel, scratch = make_kernel(n_slices, rows8, group, head_dim, key_rows, cp_size)

        def by_head(x):
            return x.transpose(0, 2, 1, 3).reshape(n_slices, kv_heads, group * rows8, head_dim)

        hbm = pl.BlockSpec(memory_space=pl.ANY)
        grad_q, grad_k, grad_v = pl.pallas_call(
            kernel,
            out_shape=(
                jax.ShapeDtypeStruct((n_slices, kv_heads, group * rows8, head_dim), jnp.bfloat16),
                jax.ShapeDtypeStruct((key_rows * kv_heads, head_dim), jnp.float32),
                jax.ShapeDtypeStruct((key_rows * kv_heads, head_dim), jnp.float32),
            ),
            in_specs=[hbm] * 6,
            out_specs=(hbm,) * 3,
            scratch_shapes=scratch,
            compiler_params=pltpu.CompilerParams(collective_id=0, has_side_effects=True, vmem_limit_bytes=60 * 2 ** 20),
        )(by_head(query_in), by_head(attn_out), by_head(grad_out), log_sum.transpose(2, 1, 0),
          key_cache.transpose(1, 0, 2), value_cache.transpose(1, 0, 2))
        grad_q = grad_q.reshape(n_slices, q_heads, rows8, head_dim).transpose(0, 2, 1, 3)
        return grad_q, grad_k.reshape(key_rows, kv_heads, head_dim), grad_v.reshape(key_rows, kv_heads, head_dim)

    return jax.shard_map(local_backward, mesh=mesh, in_specs=(row_spec, row_spec, row_spec, lse_spec, kv_spec, kv_spec), out_specs=(row_spec, kv_spec, kv_spec), check_vma=False)
```

```python
import jax
import jax.numpy as jnp
from jax import lax
from jax.experimental import pallas as pl
from jax.experimental.pallas import tpu as pltpu
from jax.sharding import PartitionSpec as P

MESH = pl.DeviceIdType.MESH
LOG2E = 1.4426950408889634
NT = (((1,), (1,)), ((), ()))
NN = (((1,), (0,)), ((), ()))
KEY_BLOCK = 256
OWN, PEER, ACROSS, DIAG = 0, 1, 2, 3
STEPS = [(0, 0), (1, 0), (0, 1), (2, 0), (3, 0), (1, 1), (2, 1), (3, 1), (0, 2), (2, 2), (3, 2), (1, 2), (2, 3), (3, 3), (0, 3), (1, 3)]
REDUCE_AT = [5, 8, 11, 14]


def dot(a, b, dims=NN):
    return lax.dot_general(a, b, dims, preferred_element_type=jnp.float32)


def table(step, values):
    out = jnp.int32(values[0])
    for i, v in enumerate(values[1:], 1):
        out = jnp.where(step == i, jnp.int32(v), out)
    return out


def make_kernel(n_slices, rows8, group, head_dim, key_rows, cp_size):
    half_slices = n_slices // 2
    unit = rows8 * group
    rows = half_slices * unit
    slice_len = rows8 * cp_size
    prefix = key_rows * cp_size - n_slices * slice_len
    n_blocks = key_rows // KEY_BLOCK
    scale = head_dim ** -0.5
    exp_scale = scale * LOG2E
    first_masked = max(0, prefix - (cp_size - 1) * key_rows) // KEY_BLOCK

    def kernel(q_hbm, o_hbm, g_hbm, l_hbm, k_hbm, v_hbm, dq_out, dk_out, dv_out,
               q_all, g_all, stat_all, o_own, lse_own, k_raw, v_raw, k_all, v_all, dk_t, dv_t, dq_all,
               from_peer_own, from_peer_across, from_across, q_t, g_t, p_a, s_a, p_b, s_b,
               lse_rep, del_rep, row_pos,
               load_sem, q_recv, g_recv, stat_recv, q_send, g_send, stat_send,
               part_recv, part_send):
        me = lax.axis_index('cp')
        chip, core = me // 2, me % 2
        peer = chip * 2 + (1 - core)
        across = (1 - chip) * 2 + core
        diag = (1 - chip) * 2 + (1 - core)

        barrier = pltpu.get_barrier_semaphore()
        for other in (peer, across):
            pl.semaphore_signal(barrier, inc=1, device_id={'cp': other}, device_id_type=MESH)

        def part(ref, ch):
            return ref.at[pl.ds((ch % 2) * half_slices, half_slices), ch // 2]

        loads = []
        for ch in range(4):
            loads.append(pltpu.make_async_copy(part(g_hbm, ch), g_all.at[OWN, ch], load_sem.at[ch]))
        for ch in range(4):
            loads.append(pltpu.make_async_copy(part(o_hbm, ch), o_own.at[ch], load_sem.at[4 + ch]))
        loads.append(pltpu.make_async_copy(l_hbm, lse_own, load_sem.at[8]))
        for ch in range(4):
            loads.append(pltpu.make_async_copy(part(q_hbm, ch), q_all.at[OWN, ch], load_sem.at[9 + ch]))
        loads.append(pltpu.make_async_copy(k_hbm, k_raw, load_sem.at[13]))
        loads.append(pltpu.make_async_copy(v_hbm, v_raw, load_sem.at[14]))
        for copy in loads:
            copy.start()

        def send_rows(ch, slot, other):
            q = pltpu.make_async_remote_copy(part(q_hbm, ch), q_all.at[slot, ch], q_send.at[slot, ch], q_recv.at[slot, ch], device_id={'cp': other}, device_id_type=MESH)
            g = pltpu.make_async_remote_copy(part(g_hbm, ch), g_all.at[slot, ch], g_send.at[slot, ch], g_recv.at[slot, ch], device_id={'cp': other}, device_id_type=MESH)
            return q, g

        def send_stat(src_slot, dst_slot, other):
            return pltpu.make_async_remote_copy(stat_all.at[src_slot], stat_all.at[dst_slot], stat_send.at[dst_slot], stat_recv.at[dst_slot], device_id={'cp': other}, device_id_type=MESH)

        def forward_rows(ch):
            q = pltpu.make_async_remote_copy(q_all.at[ACROSS, ch], q_all.at[DIAG, ch], q_send.at[DIAG, ch], q_recv.at[DIAG, ch], device_id={'cp': peer}, device_id_type=MESH)
            g = pltpu.make_async_remote_copy(g_all.at[ACROSS, ch], g_all.at[DIAG, ch], g_send.at[DIAG, ch], g_recv.at[DIAG, ch], device_id={'cp': peer}, device_id_type=MESH)
            return q, g

        def send_own_part(ch):
            return pltpu.make_async_remote_copy(dq_all.at[PEER, ch], from_peer_own.at[ch], part_send.at[0, ch], part_recv.at[0, ch], device_id={'cp': peer}, device_id_type=MESH)

        def send_diag_part(ch):
            return pltpu.make_async_remote_copy(dq_all.at[DIAG, ch], from_peer_across.at[ch], part_send.at[1, ch], part_recv.at[1, ch], device_id={'cp': peer}, device_id_type=MESH)

        def send_reduced(ch):
            return pltpu.make_async_remote_copy(dq_all.at[ACROSS, ch], from_across.at[ch], part_send.at[2, ch], part_recv.at[2, ch], device_id={'cp': across}, device_id_type=MESH)

        pl.semaphore_wait(barrier, 2)
        for slot, other in ((ACROSS, across), (PEER, peer)):
            for copy in send_rows(0, slot, other):
                copy.start()

        for copy in loads[:9]:
            copy.wait()
        lane = lax.broadcasted_iota(jnp.int32, (unit, 128), 1)
        for kv in range(2):
            acc = jnp.zeros((unit, 128), jnp.float32)
            for s in range(n_slices):
                ch = kv * 2 + s // half_slices
                prod = g_all[OWN, ch, s % half_slices].astype(jnp.float32) * o_own[ch, s % half_slices].astype(jnp.float32)
                acc = jnp.where(lane == n_slices + s, jnp.sum(prod, axis=1, keepdims=True), acc)
            stat_all[OWN, pl.ds(kv * group, group)] = acc.reshape(group, rows8, 128)
        stat_all[OWN, :, :, pl.ds(0, n_slices)] = lse_own[...] * LOG2E
        for slot, other in ((ACROSS, across), (PEER, peer)):
            send_stat(OWN, slot, other).start()
        for ch in range(1, 4):
            for slot, other in ((ACROSS, across), (PEER, peer)):
                for copy in send_rows(ch, slot, other):
                    copy.start()

        dk_t[...] = jnp.zeros_like(dk_t)
        dv_t[...] = jnp.zeros_like(dv_t)
        token = lax.broadcasted_iota(jnp.int32, (rows8, 128), 0)
        for s in range(half_slices):
            for h in range(group):
                row_pos[pl.ds((s * group + h) * rows8, rows8)] = token + s * slice_len
        for copy in loads[9:]:
            copy.wait()
        for raw, wide, split in ((k_raw, dk_out, k_all), (v_raw, dv_out, v_all)):
            for block in range(n_blocks):
                both = pl.ds(2 * block * KEY_BLOCK, 2 * KEY_BLOCK)
                wide[both] = raw[both].astype(jnp.float32)
                for kv in range(2):
                    split[kv, pl.ds(block * KEY_BLOCK, KEY_BLOCK)] = wide[pl.ds(2 * block * KEY_BLOCK + kv, KEY_BLOCK, stride=2)].astype(jnp.bfloat16)

        def step_body(step, carry):
            slot = table(step, [a for a, _ in STEPS])
            ch = table(step, [b for _, b in STEPS])
            kv, half = ch // 2, ch % 2
            source = jnp.where(slot == OWN, me, jnp.where(slot == PEER, peer, jnp.where(slot == ACROSS, across, diag)))

            @pl.when(slot != OWN)
            def _():
                pltpu.make_async_remote_copy(q_all.at[slot, ch], q_all.at[slot, ch], q_send.at[slot, ch], q_recv.at[slot, ch], device_id={'cp': peer}, device_id_type=MESH).wait_recv()
                pltpu.make_async_remote_copy(g_all.at[slot, ch], g_all.at[slot, ch], g_send.at[slot, ch], g_recv.at[slot, ch], device_id={'cp': peer}, device_id_type=MESH).wait_recv()

            @pl.when(jnp.logical_and(slot != OWN, ch == 0))
            def _():
                pltpu.make_async_remote_copy(stat_all.at[slot], stat_all.at[slot], stat_send.at[slot], stat_recv.at[slot], device_id={'cp': peer}, device_id_type=MESH).wait_recv()

            @pl.when(slot == ACROSS)
            def _():
                for copy in forward_rows(ch):
                    copy.start()

            @pl.when(jnp.logical_and(slot == ACROSS, ch == 0))
            def _():
                send_stat(ACROSS, DIAG, peer).start()

            q_t[...] = q_all[slot, ch].reshape(rows, head_dim).T
            g_t[...] = g_all[slot, ch].reshape(rows, head_dim).T
            for h in range(group):
                st = stat_all[slot, kv * group + h]
                st = jnp.where(half == 1, pltpu.roll(st, 128 - half_slices, 1), st)
                for s in range(half_slices):
                    at = pl.ds((s * group + h) * rows8, rows8)
                    lse_rep[at] = jnp.broadcast_to(st[:, s:s + 1], (rows8, 128))
                    del_rep[at] = jnp.broadcast_to(st[:, n_slices + s:n_slices + s + 1], (rows8, 128))

            def scores(block, p_buf, s_buf):
                keys = pl.ds(block * KEY_BLOCK, KEY_BLOCK)
                logits = dot(q_all[slot, ch].reshape(rows, head_dim), k_all[kv, keys], NT)
                lse = lse_rep[...]
                prob = jnp.exp2(logits * exp_scale - jnp.concatenate([lse, lse], 1))
                if block >= first_masked:
                    first = me * key_rows + block * KEY_BLOCK - prefix - half * (half_slices * slice_len) - source * rows8
                    key_pos = lax.broadcasted_iota(jnp.int32, (rows, KEY_BLOCK), 1) + first
                    pos = row_pos[...]
                    prob = jnp.where(key_pos <= jnp.concatenate([pos, pos], 1), prob, 0.0)
                grad_prob = dot(g_all[slot, ch].reshape(rows, head_dim), v_all[kv, keys], NT)
                delta = del_rep[...]
                p_buf[...] = prob.astype(jnp.bfloat16)
                s_buf[...] = (prob * (grad_prob - jnp.concatenate([delta, delta], 1))).astype(jnp.bfloat16)

            def grads(block, p_buf, s_buf):
                keys = pl.ds(block * KEY_BLOCK, KEY_BLOCK)
                dv_t[kv, :, keys] += dot(g_t[...], p_buf[...])
                dk_t[kv, :, keys] += dot(q_t[...], s_buf[...])
                part_q = dot(s_buf[...], k_all[kv, keys])
                if block == 0:
                    dq_all[slot, ch] = part_q
                else:
                    dq_all[slot, ch] += part_q

            bufs = ((p_a, s_a), (p_b, s_b))
            scores(0, *bufs[0])
            for block in range(n_blocks):
                if block + 1 < n_blocks:
                    scores(block + 1, *bufs[(block + 1) % 2])
                grads(block, *bufs[block % 2])

            @pl.when(slot == PEER)
            def _():
                send_own_part(ch).start()

            @pl.when(slot == DIAG)
            def _():
                send_diag_part(ch).start()

            reduce_ch = table(step, [REDUCE_AT.index(i) if i in REDUCE_AT else -1 for i in range(len(STEPS))])

            @pl.when(reduce_ch >= 0)
            def _():
                send_diag_part(reduce_ch).wait_recv()
                dq_all[ACROSS, reduce_ch] += from_peer_across[reduce_ch]
                send_reduced(reduce_ch).start()

            return carry

        lax.fori_loop(0, len(STEPS), step_body, 0)

        for acc_t, out, factor in ((dv_t, dv_out, None), (dk_t, dk_out, scale)):
            for block in range(n_blocks):
                for kv in range(2):
                    grad = acc_t[kv, :, pl.ds(block * KEY_BLOCK, KEY_BLOCK)].T
                    out[pl.ds(2 * block * KEY_BLOCK + kv, KEY_BLOCK, stride=2)] = grad if factor is None else grad * factor
        for ch in range(4):
            send_own_part(ch).wait_recv()
            send_reduced(ch).wait_recv()
            total = (dq_all[OWN, ch] + from_peer_own[ch] + from_across[ch]) * scale
            dq_out[pl.ds((ch % 2) * half_slices, half_slices), ch // 2] = total.astype(jnp.bfloat16).reshape(half_slices, unit, head_dim)
        for slot, other in ((ACROSS, across), (PEER, peer)):
            send_stat(OWN, slot, other).wait_send()
            for ch in range(4):
                for copy in send_rows(ch, slot, other):
                    copy.wait_send()
        send_stat(ACROSS, DIAG, peer).wait_send()
        for ch in range(4):
            for copy in forward_rows(ch):
                copy.wait_send()
            send_own_part(ch).wait_send()
            send_diag_part(ch).wait_send()
            send_reduced(ch).wait_send()

    bf16, f32 = jnp.bfloat16, jnp.float32
    chunk = (half_slices, unit, head_dim)
    scratch = [
        pltpu.VMEM((4, 4) + chunk, bf16),
        pltpu.VMEM((4, 4) + chunk, bf16),
        pltpu.VMEM((4, 2 * group, rows8, 128), f32),
        pltpu.VMEM((4,) + chunk, bf16),
        pltpu.VMEM((2 * group, rows8, n_slices), f32),
        pltpu.VMEM((2 * key_rows, head_dim), bf16),
        pltpu.VMEM((2 * key_rows, head_dim), bf16),
        pltpu.VMEM((2, key_rows, head_dim), bf16),
        pltpu.VMEM((2, key_rows, head_dim), bf16),
        pltpu.VMEM((2, head_dim, key_rows), f32),
        pltpu.VMEM((2, head_dim, key_rows), f32),
        pltpu.VMEM((4, 4, rows, head_dim), f32),
        pltpu.VMEM((4, rows, head_dim), f32),
        pltpu.VMEM((4, rows, head_dim), f32),
        pltpu.VMEM((4, rows, head_dim), f32),
        pltpu.VMEM((head_dim, rows), bf16),
        pltpu.VMEM((head_dim, rows), bf16),
        pltpu.VMEM((rows, KEY_BLOCK), bf16),
        pltpu.VMEM((rows, KEY_BLOCK), bf16),
        pltpu.VMEM((rows, KEY_BLOCK), bf16),
        pltpu.VMEM((rows, KEY_BLOCK), bf16),
        pltpu.VMEM((rows, 128), f32),
        pltpu.VMEM((rows, 128), f32),
        pltpu.VMEM((rows, 128), jnp.int32),
        pltpu.SemaphoreType.DMA((15,)),
        pltpu.SemaphoreType.DMA((4, 4)),
        pltpu.SemaphoreType.DMA((4, 4)),
        pltpu.SemaphoreType.DMA((4,)),
        pltpu.SemaphoreType.DMA((4, 4)),
        pltpu.SemaphoreType.DMA((4, 4)),
        pltpu.SemaphoreType.DMA((4,)),
        pltpu.SemaphoreType.DMA((3, 4)),
        pltpu.SemaphoreType.DMA((3, 4)),
    ]
    return kernel, scratch


def store_results(dq_in, dk_in, dv_in, dq_hbm, dk_hbm, dv_hbm, sem):
    copies = [pltpu.make_async_copy(a, b, sem.at[i]) for i, (a, b) in enumerate(((dk_in, dk_hbm), (dv_in, dv_hbm), (dq_in, dq_hbm)))]
    for copy in copies:
        copy.start()
    for copy in copies:
        copy.wait()


def solution(mesh):
    cp_size = mesh.shape['cp']
    row_spec = P(None, 'cp', 'tp', None)
    lse_spec = P(None, 'cp', 'tp')
    kv_spec = P('cp', 'tp', None)

    def local_backward(query_in, attn_out, grad_out, log_sum, key_cache, value_cache):
        n_slices, rows8, q_heads, head_dim = query_in.shape
        key_rows, kv_heads, _ = key_cache.shape
        group = q_heads // kv_heads
        kernel, scratch = make_kernel(n_slices, rows8, group, head_dim, key_rows, cp_size)

        def by_head(x):
            return x.transpose(0, 2, 1, 3).reshape(n_slices, kv_heads, group * rows8, head_dim)

        hbm, vmem = pl.BlockSpec(memory_space=pltpu.HBM), pl.BlockSpec(memory_space=pltpu.VMEM)
        grad_q, grad_k, grad_v = pl.pallas_call(
            kernel,
            out_shape=(
                jax.ShapeDtypeStruct((n_slices, kv_heads, group * rows8, head_dim), jnp.bfloat16),
                jax.ShapeDtypeStruct((key_rows * kv_heads, head_dim), jnp.float32),
                jax.ShapeDtypeStruct((key_rows * kv_heads, head_dim), jnp.float32),
            ),
            in_specs=[hbm] * 6,
            out_specs=(vmem,) * 3,
            scratch_shapes=scratch,
            compiler_params=pltpu.CompilerParams(collective_id=0, has_side_effects=True, vmem_limit_bytes=40 * 2 ** 20),
        )(*(pltpu.with_memory_space_constraint(x, pltpu.HBM) for x in (
            by_head(query_in), by_head(attn_out), by_head(grad_out), log_sum.transpose(2, 1, 0),
            key_cache.reshape(key_rows * kv_heads, head_dim), value_cache.reshape(key_rows * kv_heads, head_dim))))
        grad_q, grad_k, grad_v = pl.pallas_call(
            store_results,
            out_shape=tuple(jax.ShapeDtypeStruct(x.shape, x.dtype) for x in (grad_q, grad_k, grad_v)),
            in_specs=[vmem] * 3,
            out_specs=(hbm,) * 3,
            scratch_shapes=[pltpu.SemaphoreType.DMA((3,))],
            compiler_params=pltpu.CompilerParams(vmem_limit_bytes=2 ** 20),
        )(*(pltpu.with_memory_space_constraint(x, pltpu.VMEM) for x in (grad_q, grad_k, grad_v)))
        grad_q = grad_q.reshape(n_slices, q_heads, rows8, head_dim).transpose(0, 2, 1, 3)
        return grad_q, grad_k.reshape(key_rows, kv_heads, head_dim), grad_v.reshape(key_rows, kv_heads, head_dim)

    return jax.shard_map(local_backward, mesh=mesh, in_specs=(row_spec, row_spec, row_spec, lse_spec, kv_spec, kv_spec), out_specs=(row_spec, kv_spec, kv_spec), check_vma=False)
```

```python
import functools

import jax
import jax.numpy as jnp
from jax import lax
from jax.experimental import pallas as pl
from jax.experimental.pallas import tpu as pltpu
from jax.sharding import PartitionSpec as P

MESH = pl.DeviceIdType.MESH
LOG2E = 1.4426950408889634
NT = (((1,), (1,)), ((), ()))
NN = (((1,), (0,)), ((), ()))
KEY_BLOCK = 256
OWN, PEER, ACROSS, DIAG = 0, 1, 2, 3
STEPS = [(0, 0), (1, 0), (0, 1), (2, 0), (3, 0), (2, 1), (3, 1), (1, 1), (2, 2), (3, 2), (2, 3), (3, 3), (0, 2), (1, 2), (0, 3), (1, 3)]
REDUCE_AT = [5, 7, 10, 12]


def dot(a, b, dims=NN):
    return lax.dot_general(a, b, dims, preferred_element_type=jnp.float32)


def table(step, values):
    out = jnp.int32(values[0])
    for i, v in enumerate(values[1:], 1):
        out = jnp.where(step == i, jnp.int32(v), out)
    return out


def make_kernel(n_slices, rows8, group, head_dim, key_rows, cp_size):
    half_slices = n_slices // 2
    unit = rows8 * group
    rows = half_slices * unit
    slice_len = rows8 * cp_size
    prefix = key_rows * cp_size - n_slices * slice_len
    n_blocks = key_rows // KEY_BLOCK
    scale = head_dim ** -0.5
    exp_scale = scale * LOG2E
    last = cp_size - 1
    assert last * key_rows <= prefix

    def kernel(q_hbm, o_hbm, g_hbm, l_hbm, k_hbm, v_hbm, dq_out, dk_out, dv_out,
               q_all, g_all, stat_all, o_own, lse_own, k_raw, v_raw, k_all, v_all, dk_t, dv_t, dq_all,
               from_peer_own, from_peer_across, from_across, q_t, g_t, p_a, s_a, p_b, s_b,
               lse_rep, del_rep, row_pos,
               load_sem, q_recv, g_recv, stat_recv, q_send, g_send, stat_send,
               part_recv, part_send):
        me = lax.axis_index('cp')
        chip, core = me // 2, me % 2
        peer = chip * 2 + (1 - core)
        across = (1 - chip) * 2 + core
        diag = (1 - chip) * 2 + (1 - core)

        barrier = pltpu.get_barrier_semaphore()
        for other in (peer, across):
            pl.semaphore_signal(barrier, inc=1, device_id={'cp': other}, device_id_type=MESH)

        def part(ref, ch):
            return ref.at[pl.ds((ch % 2) * half_slices, half_slices), ch // 2]

        loads = []
        for ch in range(4):
            loads.append(pltpu.make_async_copy(part(g_hbm, ch), g_all.at[OWN, ch], load_sem.at[ch]))
        for ch in range(4):
            loads.append(pltpu.make_async_copy(part(o_hbm, ch), o_own.at[ch], load_sem.at[4 + ch]))
        loads.append(pltpu.make_async_copy(l_hbm, lse_own, load_sem.at[8]))
        for ch in range(4):
            loads.append(pltpu.make_async_copy(part(q_hbm, ch), q_all.at[OWN, ch], load_sem.at[9 + ch]))
        loads.append(pltpu.make_async_copy(k_hbm, k_raw, load_sem.at[13]))
        loads.append(pltpu.make_async_copy(v_hbm, v_raw, load_sem.at[14]))
        for copy in loads:
            copy.start()

        def send_rows(ch, slot, other):
            q = pltpu.make_async_remote_copy(part(q_hbm, ch), q_all.at[slot, ch], q_send.at[slot, ch], q_recv.at[slot, ch], device_id={'cp': other}, device_id_type=MESH)
            g = pltpu.make_async_remote_copy(part(g_hbm, ch), g_all.at[slot, ch], g_send.at[slot, ch], g_recv.at[slot, ch], device_id={'cp': other}, device_id_type=MESH)
            return q, g

        def send_stat(src_slot, dst_slot, other):
            return pltpu.make_async_remote_copy(stat_all.at[src_slot], stat_all.at[dst_slot], stat_send.at[dst_slot], stat_recv.at[dst_slot], device_id={'cp': other}, device_id_type=MESH)

        def forward_rows(ch):
            q = pltpu.make_async_remote_copy(q_all.at[ACROSS, ch], q_all.at[DIAG, ch], q_send.at[DIAG, ch], q_recv.at[DIAG, ch], device_id={'cp': peer}, device_id_type=MESH)
            g = pltpu.make_async_remote_copy(g_all.at[ACROSS, ch], g_all.at[DIAG, ch], g_send.at[DIAG, ch], g_recv.at[DIAG, ch], device_id={'cp': peer}, device_id_type=MESH)
            return q, g

        def send_own_part(ch):
            return pltpu.make_async_remote_copy(dq_all.at[PEER, ch], from_peer_own.at[ch], part_send.at[0, ch], part_recv.at[0, ch], device_id={'cp': peer}, device_id_type=MESH)

        def send_diag_part(ch):
            return pltpu.make_async_remote_copy(dq_all.at[DIAG, ch], from_peer_across.at[ch], part_send.at[1, ch], part_recv.at[1, ch], device_id={'cp': peer}, device_id_type=MESH)

        def send_reduced(ch):
            return pltpu.make_async_remote_copy(dq_all.at[ACROSS, ch], from_across.at[ch], part_send.at[2, ch], part_recv.at[2, ch], device_id={'cp': across}, device_id_type=MESH)

        pl.semaphore_wait(barrier, 2)
        for slot, other in ((ACROSS, across), (PEER, peer)):
            for copy in send_rows(0, slot, other):
                copy.start()

        for copy in loads[:9]:
            copy.wait()
        lane = lax.broadcasted_iota(jnp.int32, (unit, 128), 1)
        for kv in range(2):
            acc = jnp.zeros((unit, 128), jnp.float32)
            for s in range(n_slices):
                ch = kv * 2 + s // half_slices
                prod = g_all[OWN, ch, s % half_slices].astype(jnp.float32) * o_own[ch, s % half_slices].astype(jnp.float32)
                acc = jnp.where(lane == n_slices + s, jnp.sum(prod, axis=1, keepdims=True), acc)
            stat_all[OWN, pl.ds(kv * group, group)] = acc.reshape(group, rows8, 128)
        stat_all[OWN, :, :, pl.ds(0, n_slices)] = lse_own[...] * LOG2E
        for slot, other in ((ACROSS, across), (PEER, peer)):
            send_stat(OWN, slot, other).start()
        for ch in range(1, 4):
            for slot, other in ((ACROSS, across), (PEER, peer)):
                for copy in send_rows(ch, slot, other):
                    copy.start()

        dk_t[...] = jnp.zeros_like(dk_t)
        dv_t[...] = jnp.zeros_like(dv_t)
        token = lax.broadcasted_iota(jnp.int32, (rows8, 128), 0)
        for s in range(half_slices):
            for h in range(group):
                row_pos[pl.ds((s * group + h) * rows8, rows8)] = token + s * slice_len
        for copy in loads[9:]:
            copy.wait()
        for raw, wide, split in ((k_raw, dk_out, k_all), (v_raw, dv_out, v_all)):
            for block in range(n_blocks):
                both = pl.ds(2 * block * KEY_BLOCK, 2 * KEY_BLOCK)
                wide[both] = raw[both].astype(jnp.float32)
                for kv in range(2):
                    split[kv, pl.ds(block * KEY_BLOCK, KEY_BLOCK)] = wide[pl.ds(2 * block * KEY_BLOCK + kv, KEY_BLOCK, stride=2)].astype(jnp.bfloat16)

        def step_body(on_last, step, carry):
            slot = table(step, [a for a, _ in STEPS])
            ch = table(step, [b for _, b in STEPS])
            kv, half = ch // 2, ch % 2
            source = jnp.where(slot == OWN, me, jnp.where(slot == PEER, peer, jnp.where(slot == ACROSS, across, diag)))

            @pl.when(slot != OWN)
            def _():
                pltpu.make_async_remote_copy(q_all.at[slot, ch], q_all.at[slot, ch], q_send.at[slot, ch], q_recv.at[slot, ch], device_id={'cp': peer}, device_id_type=MESH).wait_recv()
                pltpu.make_async_remote_copy(g_all.at[slot, ch], g_all.at[slot, ch], g_send.at[slot, ch], g_recv.at[slot, ch], device_id={'cp': peer}, device_id_type=MESH).wait_recv()

            @pl.when(jnp.logical_and(slot != OWN, ch == 0))
            def _():
                pltpu.make_async_remote_copy(stat_all.at[slot], stat_all.at[slot], stat_send.at[slot], stat_recv.at[slot], device_id={'cp': peer}, device_id_type=MESH).wait_recv()

            @pl.when(slot == ACROSS)
            def _():
                for copy in forward_rows(ch):
                    copy.start()

            @pl.when(jnp.logical_and(slot == ACROSS, ch == 0))
            def _():
                send_stat(ACROSS, DIAG, peer).start()

            q_t[...] = q_all[slot, ch].reshape(rows, head_dim).T
            g_t[...] = g_all[slot, ch].reshape(rows, head_dim).T
            for h in range(group):
                st = stat_all[slot, kv * group + h]
                st = jnp.where(half == 1, pltpu.roll(st, 128 - half_slices, 1), st)
                for s in range(half_slices):
                    at = pl.ds((s * group + h) * rows8, rows8)
                    lse_rep[at] = jnp.broadcast_to(st[:, s:s + 1], (rows8, 128))
                    del_rep[at] = jnp.broadcast_to(st[:, n_slices + s:n_slices + s + 1], (rows8, 128))

            def scores(block, p_buf, s_buf, masked):
                keys = pl.ds(block * KEY_BLOCK, KEY_BLOCK)
                logits = dot(q_all[slot, ch].reshape(rows, head_dim), k_all[kv, keys], NT)
                lse = lse_rep[...]
                prob = jnp.exp2(logits * exp_scale - jnp.concatenate([lse, lse], 1))
                if masked:
                    first = me * key_rows + block * KEY_BLOCK - prefix - half * (half_slices * slice_len) - source * rows8
                    key_pos = lax.broadcasted_iota(jnp.int32, (rows, KEY_BLOCK), 1) + first
                    pos = row_pos[...]
                    prob = jnp.where(key_pos <= jnp.concatenate([pos, pos], 1), prob, 0.0)
                grad_prob = dot(g_all[slot, ch].reshape(rows, head_dim), v_all[kv, keys], NT)
                delta = del_rep[...]
                p_buf[...] = prob.astype(jnp.bfloat16)
                s_buf[...] = (prob * (grad_prob - jnp.concatenate([delta, delta], 1))).astype(jnp.bfloat16)

            def grads(block, p_buf, s_buf):
                keys = pl.ds(block * KEY_BLOCK, KEY_BLOCK)
                dv_t[kv, :, keys] += dot(g_t[...], p_buf[...])
                dk_t[kv, :, keys] += dot(q_t[...], s_buf[...])
                part_q = dot(s_buf[...], k_all[kv, keys])
                if block == 0:
                    dq_all[slot, ch] = part_q
                else:
                    dq_all[slot, ch] += part_q

            bufs = ((p_a, s_a), (p_b, s_b))

            masked = [on_last and last * key_rows + (block + 1) * KEY_BLOCK > prefix for block in range(n_blocks)]
            scores(0, *bufs[0], masked[0])
            for block in range(n_blocks):
                if block + 1 < n_blocks:
                    scores(block + 1, *bufs[(block + 1) % 2], masked[block + 1])
                grads(block, *bufs[block % 2])

            @pl.when(slot == PEER)
            def _():
                send_own_part(ch).start()

            @pl.when(slot == DIAG)
            def _():
                send_diag_part(ch).start()

            reduce_ch = table(step, [REDUCE_AT.index(i) if i in REDUCE_AT else -1 for i in range(len(STEPS))])

            @pl.when(reduce_ch >= 0)
            def _():
                send_diag_part(reduce_ch).wait_recv()
                dq_all[ACROSS, reduce_ch] += from_peer_across[reduce_ch]
                send_reduced(reduce_ch).start()

            return carry

        for on_last in (False, True):
            @pl.when((me == last) == on_last)
            def _(on_last=on_last):
                lax.fori_loop(0, len(STEPS), functools.partial(step_body, on_last), 0)

        for acc_t, out, factor in ((dv_t, dv_out, None), (dk_t, dk_out, scale)):
            for block in range(n_blocks):
                for kv in range(2):
                    grad = acc_t[kv, :, pl.ds(block * KEY_BLOCK, KEY_BLOCK)].T
                    out[pl.ds(2 * block * KEY_BLOCK + kv, KEY_BLOCK, stride=2)] = grad if factor is None else grad * factor
        for ch in range(4):
            send_own_part(ch).wait_recv()
            send_reduced(ch).wait_recv()
            total = (dq_all[OWN, ch] + from_peer_own[ch] + from_across[ch]) * scale
            dq_out[pl.ds((ch % 2) * half_slices, half_slices), ch // 2] = total.astype(jnp.bfloat16).reshape(half_slices, unit, head_dim)
        for slot, other in ((ACROSS, across), (PEER, peer)):
            send_stat(OWN, slot, other).wait_send()
            for ch in range(4):
                for copy in send_rows(ch, slot, other):
                    copy.wait_send()
        send_stat(ACROSS, DIAG, peer).wait_send()
        for ch in range(4):
            for copy in forward_rows(ch):
                copy.wait_send()
            send_own_part(ch).wait_send()
            send_diag_part(ch).wait_send()
            send_reduced(ch).wait_send()

    bf16, f32 = jnp.bfloat16, jnp.float32
    chunk = (half_slices, unit, head_dim)
    scratch = [
        pltpu.VMEM((4, 4) + chunk, bf16),
        pltpu.VMEM((4, 4) + chunk, bf16),
        pltpu.VMEM((4, 2 * group, rows8, 128), f32),
        pltpu.VMEM((4,) + chunk, bf16),
        pltpu.VMEM((2 * group, rows8, n_slices), f32),
        pltpu.VMEM((2 * key_rows, head_dim), bf16),
        pltpu.VMEM((2 * key_rows, head_dim), bf16),
        pltpu.VMEM((2, key_rows, head_dim), bf16),
        pltpu.VMEM((2, key_rows, head_dim), bf16),
        pltpu.VMEM((2, head_dim, key_rows), f32),
        pltpu.VMEM((2, head_dim, key_rows), f32),
        pltpu.VMEM((4, 4, rows, head_dim), f32),
        pltpu.VMEM((4, rows, head_dim), f32),
        pltpu.VMEM((4, rows, head_dim), f32),
        pltpu.VMEM((4, rows, head_dim), f32),
        pltpu.VMEM((head_dim, rows), bf16),
        pltpu.VMEM((head_dim, rows), bf16),
        pltpu.VMEM((rows, KEY_BLOCK), bf16),
        pltpu.VMEM((rows, KEY_BLOCK), bf16),
        pltpu.VMEM((rows, KEY_BLOCK), bf16),
        pltpu.VMEM((rows, KEY_BLOCK), bf16),
        pltpu.VMEM((rows, 128), f32),
        pltpu.VMEM((rows, 128), f32),
        pltpu.VMEM((rows, 128), jnp.int32),
        pltpu.SemaphoreType.DMA((15,)),
        pltpu.SemaphoreType.DMA((4, 4)),
        pltpu.SemaphoreType.DMA((4, 4)),
        pltpu.SemaphoreType.DMA((4,)),
        pltpu.SemaphoreType.DMA((4, 4)),
        pltpu.SemaphoreType.DMA((4, 4)),
        pltpu.SemaphoreType.DMA((4,)),
        pltpu.SemaphoreType.DMA((3, 4)),
        pltpu.SemaphoreType.DMA((3, 4)),
    ]
    return kernel, scratch


def store_results(dq_in, dk_in, dv_in, dq_hbm, dk_hbm, dv_hbm, sem):
    copies = [pltpu.make_async_copy(a, b, sem.at[i]) for i, (a, b) in enumerate(((dk_in, dk_hbm), (dv_in, dv_hbm), (dq_in, dq_hbm)))]
    for copy in copies:
        copy.start()
    for copy in copies:
        copy.wait()


def solution(mesh):
    cp_size = mesh.shape['cp']
    row_spec = P(None, 'cp', 'tp', None)
    lse_spec = P(None, 'cp', 'tp')
    kv_spec = P('cp', 'tp', None)

    def local_backward(query_in, attn_out, grad_out, log_sum, key_cache, value_cache):
        n_slices, rows8, q_heads, head_dim = query_in.shape
        key_rows, kv_heads, _ = key_cache.shape
        group = q_heads // kv_heads
        kernel, scratch = make_kernel(n_slices, rows8, group, head_dim, key_rows, cp_size)

        def by_head(x):
            return x.transpose(0, 2, 1, 3).reshape(n_slices, kv_heads, group * rows8, head_dim)

        hbm, vmem = pl.BlockSpec(memory_space=pltpu.HBM), pl.BlockSpec(memory_space=pltpu.VMEM)
        grad_q, grad_k, grad_v = pl.pallas_call(
            kernel,
            out_shape=(
                jax.ShapeDtypeStruct((n_slices, kv_heads, group * rows8, head_dim), jnp.bfloat16),
                jax.ShapeDtypeStruct((key_rows * kv_heads, head_dim), jnp.float32),
                jax.ShapeDtypeStruct((key_rows * kv_heads, head_dim), jnp.float32),
            ),
            in_specs=[hbm] * 6,
            out_specs=(vmem,) * 3,
            scratch_shapes=scratch,
            compiler_params=pltpu.CompilerParams(collective_id=0, has_side_effects=True, vmem_limit_bytes=40 * 2 ** 20),
        )(*(pltpu.with_memory_space_constraint(x, pltpu.HBM) for x in (
            by_head(query_in), by_head(attn_out), by_head(grad_out), log_sum.transpose(2, 1, 0),
            key_cache.reshape(key_rows * kv_heads, head_dim), value_cache.reshape(key_rows * kv_heads, head_dim))))
        grad_q, grad_k, grad_v = pl.pallas_call(
            store_results,
            out_shape=tuple(jax.ShapeDtypeStruct(x.shape, x.dtype) for x in (grad_q, grad_k, grad_v)),
            in_specs=[vmem] * 3,
            out_specs=(hbm,) * 3,
            scratch_shapes=[pltpu.SemaphoreType.DMA((3,))],
            compiler_params=pltpu.CompilerParams(vmem_limit_bytes=2 ** 20),
        )(*(pltpu.with_memory_space_constraint(x, pltpu.VMEM) for x in (grad_q, grad_k, grad_v)))
        grad_q = grad_q.reshape(n_slices, q_heads, rows8, head_dim).transpose(0, 2, 1, 3)
        return grad_q, grad_k.reshape(key_rows, kv_heads, head_dim), grad_v.reshape(key_rows, kv_heads, head_dim)

    return jax.shard_map(local_backward, mesh=mesh, in_specs=(row_spec, row_spec, row_spec, lse_spec, kv_spec, kv_spec), out_specs=(row_spec, kv_spec, kv_spec), check_vma=False)
```

```python
import functools

import jax
import jax.numpy as jnp
from jax import lax
from jax.experimental import pallas as pl
from jax.experimental.pallas import tpu as pltpu
from jax.sharding import PartitionSpec as P

MESH = pl.DeviceIdType.MESH
LOG2E = 1.4426950408889634
NT = (((1,), (1,)), ((), ()))
NN = (((1,), (0,)), ((), ()))
KEY_BLOCK = 256
OWN, PEER, ACROSS, DIAG = 0, 1, 2, 3
STEPS = [(0, 0), (1, 0), (0, 1), (2, 0), (3, 0), (2, 1), (3, 1), (1, 1), (2, 2), (3, 2), (2, 3), (3, 3), (0, 2), (1, 2), (0, 3), (1, 3)]
REDUCE_AT = [5, 7, 10, 12]


def dot(a, b, dims=NN):
    return lax.dot_general(a, b, dims, preferred_element_type=jnp.float32)


def table(step, values):
    out = jnp.int32(values[0])
    for i, v in enumerate(values[1:], 1):
        out = jnp.where(step == i, jnp.int32(v), out)
    return out


def make_kernel(n_slices, rows8, group, head_dim, key_rows, cp_size):
    half_slices = n_slices // 2
    unit = rows8 * group
    rows = half_slices * unit
    slice_len = rows8 * cp_size
    prefix = key_rows * cp_size - n_slices * slice_len
    n_blocks = key_rows // KEY_BLOCK
    scale = head_dim ** -0.5
    exp_scale = scale * LOG2E
    last = cp_size - 1
    assert last * key_rows <= prefix

    def kernel(q_hbm, o_hbm, g_hbm, l_hbm, k_hbm, v_hbm, dq_out, dk_out, dv_out,
               q_all, g_all, stat_all, stat_pack, o_own, lse_own, lse_wide, k_raw, v_raw, k_all, v_all, dk_t, dv_t, dq_all,
               from_peer_own, from_peer_across, from_across, q_t, g_t, p_a, s_a, p_b, s_b,
               lse_rep, del_rep, row_pos,
               load_sem, q_recv, g_recv, stat_recv, q_send, g_send, stat_send,
               part_recv, part_send):
        me = lax.axis_index('cp')
        chip, core = me // 2, me % 2
        peer = chip * 2 + (1 - core)
        across = (1 - chip) * 2 + core
        diag = (1 - chip) * 2 + (1 - core)

        barrier = pltpu.get_barrier_semaphore()
        for other in (peer, across):
            pl.semaphore_signal(barrier, inc=1, device_id={'cp': other}, device_id_type=MESH)

        def part(ref, ch):
            return ref.at[pl.ds((ch % 2) * half_slices, half_slices), ch // 2]

        loads = []
        for ch in range(4):
            loads.append(pltpu.make_async_copy(part(g_hbm, ch), g_all.at[OWN, ch], load_sem.at[ch]))
        for ch in range(4):
            loads.append(pltpu.make_async_copy(part(o_hbm, ch), o_own.at[ch], load_sem.at[4 + ch]))
        loads.append(pltpu.make_async_copy(l_hbm, lse_own, load_sem.at[8]))
        for ch in range(4):
            loads.append(pltpu.make_async_copy(part(q_hbm, ch), q_all.at[OWN, ch], load_sem.at[9 + ch]))
        loads.append(pltpu.make_async_copy(k_hbm, k_raw, load_sem.at[13]))
        loads.append(pltpu.make_async_copy(v_hbm, v_raw, load_sem.at[14]))
        for copy in loads:
            copy.start()

        def send_rows(ch, slot, other):
            q = pltpu.make_async_remote_copy(part(q_hbm, ch), q_all.at[slot, ch], q_send.at[slot, ch], q_recv.at[slot, ch], device_id={'cp': other}, device_id_type=MESH)
            g = pltpu.make_async_remote_copy(part(g_hbm, ch), g_all.at[slot, ch], g_send.at[slot, ch], g_recv.at[slot, ch], device_id={'cp': other}, device_id_type=MESH)
            return q, g

        def send_stat(src_slot, dst_slot, other):
            return pltpu.make_async_remote_copy(stat_pack.at[src_slot], stat_pack.at[dst_slot], stat_send.at[dst_slot], stat_recv.at[dst_slot], device_id={'cp': other}, device_id_type=MESH)

        def forward_rows(ch):
            q = pltpu.make_async_remote_copy(q_all.at[ACROSS, ch], q_all.at[DIAG, ch], q_send.at[DIAG, ch], q_recv.at[DIAG, ch], device_id={'cp': peer}, device_id_type=MESH)
            g = pltpu.make_async_remote_copy(g_all.at[ACROSS, ch], g_all.at[DIAG, ch], g_send.at[DIAG, ch], g_recv.at[DIAG, ch], device_id={'cp': peer}, device_id_type=MESH)
            return q, g

        def send_own_part(ch):
            return pltpu.make_async_remote_copy(dq_all.at[PEER, ch], from_peer_own.at[ch], part_send.at[0, ch], part_recv.at[0, ch], device_id={'cp': peer}, device_id_type=MESH)

        def send_diag_part(ch):
            return pltpu.make_async_remote_copy(dq_all.at[DIAG, ch], from_peer_across.at[ch], part_send.at[1, ch], part_recv.at[1, ch], device_id={'cp': peer}, device_id_type=MESH)

        def send_reduced(ch):
            return pltpu.make_async_remote_copy(dq_all.at[ACROSS, ch], from_across.at[ch], part_send.at[2, ch], part_recv.at[2, ch], device_id={'cp': across}, device_id_type=MESH)

        def unpack_stats(slot):
            both = stat_pack[slot].reshape(unit, 128)
            stat_all[slot, pl.ds(0, group)] = both.reshape(group, rows8, 128)
            stat_all[slot, pl.ds(group, group)] = pltpu.roll(both, 128 - 2 * n_slices, 1).reshape(group, rows8, 128)

        pl.semaphore_wait(barrier, 2)

        def start_rows(ch, slot, other):
            for copy in send_rows(ch, slot, other):
                copy.start()

        pl.when(core == 0)(lambda: start_rows(0, ACROSS, across))
        start_rows(0, PEER, peer)

        for copy in loads[:9]:
            copy.wait()
        lane = lax.broadcasted_iota(jnp.int32, (unit, 128), 1)
        lse_wide[...] = jnp.zeros_like(lse_wide)
        lse_wide[:, :, pl.ds(0, n_slices)] = lse_own[...] * LOG2E
        stats = []
        for kv in range(2):
            acc = jnp.zeros((unit, 128), jnp.float32)
            for s in range(n_slices):
                ch = kv * 2 + s // half_slices
                prod = g_all[OWN, ch, s % half_slices].astype(jnp.float32) * o_own[ch, s % half_slices].astype(jnp.float32)
                acc = jnp.where(lane == 2 * n_slices * kv + n_slices + s, jnp.sum(prod, axis=1, keepdims=True), acc)
            lse = lse_wide[pl.ds(kv * group, group)].reshape(unit, 128)
            stats.append(jnp.where(lane % (2 * n_slices) < n_slices, pltpu.roll(lse, 2 * n_slices, 1) if kv else lse, acc))
        stat_pack[OWN] = jnp.where(lane < 2 * n_slices, stats[0], stats[1]).reshape(group, rows8, 128)
        pl.when(core == 1)(lambda: start_rows(0, ACROSS, across))
        for slot, other in ((ACROSS, across), (PEER, peer)):
            send_stat(OWN, slot, other).start()
        for ch in range(1, 4):
            for slot, other in ((ACROSS, across), (PEER, peer)):
                start_rows(ch, slot, other)

        unpack_stats(OWN)
        dk_t[...] = jnp.zeros_like(dk_t)
        dv_t[...] = jnp.zeros_like(dv_t)
        token = lax.broadcasted_iota(jnp.int32, (rows8, 128), 0)
        for s in range(half_slices):
            for h in range(group):
                row_pos[pl.ds((s * group + h) * rows8, rows8)] = token + s * slice_len
        for copy in loads[9:]:
            copy.wait()
        for raw, wide, split in ((k_raw, dk_out, k_all), (v_raw, dv_out, v_all)):
            for block in range(n_blocks):
                both = pl.ds(2 * block * KEY_BLOCK, 2 * KEY_BLOCK)
                wide[both] = raw[both].astype(jnp.float32)
                for kv in range(2):
                    split[kv, pl.ds(block * KEY_BLOCK, KEY_BLOCK)] = wide[pl.ds(2 * block * KEY_BLOCK + kv, KEY_BLOCK, stride=2)].astype(jnp.bfloat16)

        def step_body(on_last, step, carry):
            slot = table(step, [a for a, _ in STEPS])
            ch = table(step, [b for _, b in STEPS])
            kv, half = ch // 2, ch % 2
            source = jnp.where(slot == OWN, me, jnp.where(slot == PEER, peer, jnp.where(slot == ACROSS, across, diag)))

            @pl.when(slot != OWN)
            def _():
                pltpu.make_async_remote_copy(q_all.at[slot, ch], q_all.at[slot, ch], q_send.at[slot, ch], q_recv.at[slot, ch], device_id={'cp': peer}, device_id_type=MESH).wait_recv()
                pltpu.make_async_remote_copy(g_all.at[slot, ch], g_all.at[slot, ch], g_send.at[slot, ch], g_recv.at[slot, ch], device_id={'cp': peer}, device_id_type=MESH).wait_recv()

            @pl.when(jnp.logical_and(slot != OWN, ch == 0))
            def _():
                pltpu.make_async_remote_copy(stat_pack.at[slot], stat_pack.at[slot], stat_send.at[slot], stat_recv.at[slot], device_id={'cp': peer}, device_id_type=MESH).wait_recv()
                unpack_stats(slot)

            @pl.when(slot == ACROSS)
            def _():
                for copy in forward_rows(ch):
                    copy.start()

            @pl.when(jnp.logical_and(slot == ACROSS, ch == 0))
            def _():
                send_stat(ACROSS, DIAG, peer).start()

            q_t[...] = q_all[slot, ch].reshape(rows, head_dim).T
            g_t[...] = g_all[slot, ch].reshape(rows, head_dim).T
            for h in range(group):
                st = stat_all[slot, kv * group + h]
                st = jnp.where(half == 1, pltpu.roll(st, 128 - half_slices, 1), st)
                for s in range(half_slices):
                    at = pl.ds((s * group + h) * rows8, rows8)
                    lse_rep[at] = jnp.broadcast_to(st[:, s:s + 1], (rows8, 128))
                    del_rep[at] = jnp.broadcast_to(st[:, n_slices + s:n_slices + s + 1], (rows8, 128))

            def scores(block, p_buf, s_buf, masked):
                keys = pl.ds(block * KEY_BLOCK, KEY_BLOCK)
                logits = dot(q_all[slot, ch].reshape(rows, head_dim), k_all[kv, keys], NT)
                lse = lse_rep[...]
                prob = jnp.exp2(logits * exp_scale - jnp.concatenate([lse, lse], 1))
                if masked:
                    first = me * key_rows + block * KEY_BLOCK - prefix - half * (half_slices * slice_len) - source * rows8
                    key_pos = lax.broadcasted_iota(jnp.int32, (rows, KEY_BLOCK), 1) + first
                    pos = row_pos[...]
                    prob = jnp.where(key_pos <= jnp.concatenate([pos, pos], 1), prob, 0.0)
                grad_prob = dot(g_all[slot, ch].reshape(rows, head_dim), v_all[kv, keys], NT)
                delta = del_rep[...]
                p_buf[...] = prob.astype(jnp.bfloat16)
                s_buf[...] = (prob * (grad_prob - jnp.concatenate([delta, delta], 1))).astype(jnp.bfloat16)

            def grads(block, p_buf, s_buf):
                keys = pl.ds(block * KEY_BLOCK, KEY_BLOCK)
                dv_t[kv, :, keys] += dot(g_t[...], p_buf[...])
                dk_t[kv, :, keys] += dot(q_t[...], s_buf[...])
                part_q = dot(s_buf[...], k_all[kv, keys])
                if block == 0:
                    dq_all[slot, ch] = part_q
                else:
                    dq_all[slot, ch] += part_q

            bufs = ((p_a, s_a), (p_b, s_b))

            masked = [on_last and last * key_rows + (block + 1) * KEY_BLOCK > prefix for block in range(n_blocks)]
            scores(0, *bufs[0], masked[0])
            for block in range(n_blocks):
                if block + 1 < n_blocks:
                    scores(block + 1, *bufs[(block + 1) % 2], masked[block + 1])
                grads(block, *bufs[block % 2])

            @pl.when(slot == PEER)
            def _():
                send_own_part(ch).start()

            @pl.when(slot == DIAG)
            def _():
                send_diag_part(ch).start()

            reduce_ch = table(step, [REDUCE_AT.index(i) if i in REDUCE_AT else -1 for i in range(len(STEPS))])

            @pl.when(reduce_ch >= 0)
            def _():
                send_diag_part(reduce_ch).wait_recv()
                dq_all[ACROSS, reduce_ch] += from_peer_across[reduce_ch]
                send_reduced(reduce_ch).start()

            return carry

        for on_last in (False, True):
            @pl.when((me == last) == on_last)
            def _(on_last=on_last):
                lax.fori_loop(0, len(STEPS), functools.partial(step_body, on_last), 0)

        for acc_t, out, factor in ((dv_t, dv_out, None), (dk_t, dk_out, scale)):
            for block in range(n_blocks):
                for kv in range(2):
                    grad = acc_t[kv, :, pl.ds(block * KEY_BLOCK, KEY_BLOCK)].T
                    out[pl.ds(2 * block * KEY_BLOCK + kv, KEY_BLOCK, stride=2)] = grad if factor is None else grad * factor
        for ch in range(4):
            send_own_part(ch).wait_recv()
            send_reduced(ch).wait_recv()
            total = (dq_all[OWN, ch] + from_peer_own[ch] + from_across[ch]) * scale
            dq_out[pl.ds((ch % 2) * half_slices, half_slices), ch // 2] = total.astype(jnp.bfloat16).reshape(half_slices, unit, head_dim)
        for slot, other in ((ACROSS, across), (PEER, peer)):
            send_stat(OWN, slot, other).wait_send()
            for ch in range(4):
                for copy in send_rows(ch, slot, other):
                    copy.wait_send()
        send_stat(ACROSS, DIAG, peer).wait_send()
        for ch in range(4):
            for copy in forward_rows(ch):
                copy.wait_send()
            send_own_part(ch).wait_send()
            send_diag_part(ch).wait_send()
            send_reduced(ch).wait_send()

    bf16, f32 = jnp.bfloat16, jnp.float32
    chunk = (half_slices, unit, head_dim)
    scratch = [
        pltpu.VMEM((4, 4) + chunk, bf16),
        pltpu.VMEM((4, 4) + chunk, bf16),
        pltpu.VMEM((4, 2 * group, rows8, 128), f32),
        pltpu.VMEM((4, group, rows8, 128), f32),
        pltpu.VMEM((4,) + chunk, bf16),
        pltpu.VMEM((2 * group, rows8, n_slices), f32),
        pltpu.VMEM((2 * group, rows8, 128), f32),
        pltpu.VMEM((2 * key_rows, head_dim), bf16),
        pltpu.VMEM((2 * key_rows, head_dim), bf16),
        pltpu.VMEM((2, key_rows, head_dim), bf16),
        pltpu.VMEM((2, key_rows, head_dim), bf16),
        pltpu.VMEM((2, head_dim, key_rows), f32),
        pltpu.VMEM((2, head_dim, key_rows), f32),
        pltpu.VMEM((4, 4, rows, head_dim), f32),
        pltpu.VMEM((4, rows, head_dim), f32),
        pltpu.VMEM((4, rows, head_dim), f32),
        pltpu.VMEM((4, rows, head_dim), f32),
        pltpu.VMEM((head_dim, rows), bf16),
        pltpu.VMEM((head_dim, rows), bf16),
        pltpu.VMEM((rows, KEY_BLOCK), bf16),
        pltpu.VMEM((rows, KEY_BLOCK), bf16),
        pltpu.VMEM((rows, KEY_BLOCK), bf16),
        pltpu.VMEM((rows, KEY_BLOCK), bf16),
        pltpu.VMEM((rows, 128), f32),
        pltpu.VMEM((rows, 128), f32),
        pltpu.VMEM((rows, 128), jnp.int32),
        pltpu.SemaphoreType.DMA((15,)),
        pltpu.SemaphoreType.DMA((4, 4)),
        pltpu.SemaphoreType.DMA((4, 4)),
        pltpu.SemaphoreType.DMA((4,)),
        pltpu.SemaphoreType.DMA((4, 4)),
        pltpu.SemaphoreType.DMA((4, 4)),
        pltpu.SemaphoreType.DMA((4,)),
        pltpu.SemaphoreType.DMA((3, 4)),
        pltpu.SemaphoreType.DMA((3, 4)),
    ]
    return kernel, scratch


def store_results(dq_in, dk_in, dv_in, dq_hbm, dk_hbm, dv_hbm, sem):
    copies = [pltpu.make_async_copy(a, b, sem.at[i]) for i, (a, b) in enumerate(((dk_in, dk_hbm), (dv_in, dv_hbm), (dq_in, dq_hbm)))]
    for copy in copies:
        copy.start()
    for copy in copies:
        copy.wait()


def solution(mesh):
    cp_size = mesh.shape['cp']
    row_spec = P(None, 'cp', 'tp', None)
    lse_spec = P(None, 'cp', 'tp')
    kv_spec = P('cp', 'tp', None)

    def local_backward(query_in, attn_out, grad_out, log_sum, key_cache, value_cache):
        n_slices, rows8, q_heads, head_dim = query_in.shape
        key_rows, kv_heads, _ = key_cache.shape
        group = q_heads // kv_heads
        kernel, scratch = make_kernel(n_slices, rows8, group, head_dim, key_rows, cp_size)

        def by_head(x):
            return x.transpose(0, 2, 1, 3).reshape(n_slices, kv_heads, group * rows8, head_dim)

        hbm, vmem = pl.BlockSpec(memory_space=pltpu.HBM), pl.BlockSpec(memory_space=pltpu.VMEM)
        grad_q, grad_k, grad_v = pl.pallas_call(
            kernel,
            out_shape=(
                jax.ShapeDtypeStruct((n_slices, kv_heads, group * rows8, head_dim), jnp.bfloat16),
                jax.ShapeDtypeStruct((key_rows * kv_heads, head_dim), jnp.float32),
                jax.ShapeDtypeStruct((key_rows * kv_heads, head_dim), jnp.float32),
            ),
            in_specs=[hbm] * 6,
            out_specs=(vmem,) * 3,
            scratch_shapes=scratch,
            compiler_params=pltpu.CompilerParams(collective_id=0, has_side_effects=True, vmem_limit_bytes=40 * 2 ** 20),
        )(*(pltpu.with_memory_space_constraint(x, pltpu.HBM) for x in (
            by_head(query_in), by_head(attn_out), by_head(grad_out), log_sum.transpose(2, 1, 0),
            key_cache.reshape(key_rows * kv_heads, head_dim), value_cache.reshape(key_rows * kv_heads, head_dim))))
        grad_q, grad_k, grad_v = pl.pallas_call(
            store_results,
            out_shape=tuple(jax.ShapeDtypeStruct(x.shape, x.dtype) for x in (grad_q, grad_k, grad_v)),
            in_specs=[vmem] * 3,
            out_specs=(hbm,) * 3,
            scratch_shapes=[pltpu.SemaphoreType.DMA((3,))],
            compiler_params=pltpu.CompilerParams(vmem_limit_bytes=2 ** 20),
        )(*(pltpu.with_memory_space_constraint(x, pltpu.VMEM) for x in (grad_q, grad_k, grad_v)))
        grad_q = grad_q.reshape(n_slices, q_heads, rows8, head_dim).transpose(0, 2, 1, 3)
        return grad_q, grad_k.reshape(key_rows, kv_heads, head_dim), grad_v.reshape(key_rows, kv_heads, head_dim)

    return jax.shard_map(local_backward, mesh=mesh, in_specs=(row_spec, row_spec, row_spec, lse_spec, kv_spec, kv_spec), out_specs=(row_spec, kv_spec, kv_spec), check_vma=False)
```

```python
import functools

import jax
import jax.numpy as jnp
from jax import lax
from jax.experimental import pallas as pl
from jax.experimental.pallas import tpu as pltpu
from jax.sharding import PartitionSpec as P

MESH = pl.DeviceIdType.MESH
LOG2E = 1.4426950408889634
NT = (((1,), (1,)), ((), ()))
NN = (((1,), (0,)), ((), ()))
KEY_BLOCK = 256
OWN, PEER, ACROSS, DIAG = 0, 1, 2, 3
STEPS = [(0, 0), (1, 0), (0, 1), (2, 0), (3, 0), (2, 1), (3, 1), (1, 1), (2, 2), (3, 2), (2, 3), (3, 3), (0, 2), (1, 2), (0, 3), (1, 3)]
REDUCE_AT = [5, 7, 10, 12]
REDUCE_NEAR = [5, 7, 10, 14]


def dot(a, b, dims=NN):
    return lax.dot_general(a, b, dims, preferred_element_type=jnp.float32)


def table(step, values):
    out = jnp.int32(values[0])
    for i, v in enumerate(values[1:], 1):
        out = jnp.where(step == i, jnp.int32(v), out)
    return out


def make_kernel(n_slices, rows8, group, head_dim, key_rows, cp_size):
    half_slices = n_slices // 2
    unit = rows8 * group
    rows = half_slices * unit
    slice_len = rows8 * cp_size
    prefix = key_rows * cp_size - n_slices * slice_len
    n_blocks = key_rows // KEY_BLOCK
    scale = head_dim ** -0.5
    exp_scale = scale * LOG2E
    last = cp_size - 1
    assert last * key_rows <= prefix

    def kernel(q_hbm, o_hbm, g_hbm, l_hbm, k_hbm, v_hbm, dq_out, dk_out, dv_out,
               q_all, g_all, stat_all, stat_pack, o_own, lse_own, lse_wide, k_raw, v_raw, k_all, v_all, dk_t, dv_t, dq_all,
               from_peer_own, from_peer_across, from_across, q_t, g_t, p_a, s_a, p_b, s_b,
               lse_rep, del_rep, row_pos,
               load_sem, q_recv, g_recv, stat_recv, q_send, g_send, stat_send,
               part_recv, part_send):
        me = lax.axis_index('cp')
        chip, core = me // 2, me % 2
        peer = chip * 2 + (1 - core)
        across = (1 - chip) * 2 + core
        diag = (1 - chip) * 2 + (1 - core)

        barrier = pltpu.get_barrier_semaphore()
        for other in (peer, across):
            pl.semaphore_signal(barrier, inc=1, device_id={'cp': other}, device_id_type=MESH)

        def part(ref, ch):
            return ref.at[pl.ds((ch % 2) * half_slices, half_slices), ch // 2]

        loads = []
        for ch in range(4):
            loads.append(pltpu.make_async_copy(part(g_hbm, ch), g_all.at[OWN, ch], load_sem.at[ch]))
        for ch in range(4):
            loads.append(pltpu.make_async_copy(part(o_hbm, ch), o_own.at[ch], load_sem.at[4 + ch]))
        loads.append(pltpu.make_async_copy(l_hbm, lse_own, load_sem.at[8]))
        for ch in range(4):
            loads.append(pltpu.make_async_copy(part(q_hbm, ch), q_all.at[OWN, ch], load_sem.at[9 + ch]))
        loads.append(pltpu.make_async_copy(k_hbm, k_raw, load_sem.at[13]))
        loads.append(pltpu.make_async_copy(v_hbm, v_raw, load_sem.at[14]))
        for copy in loads:
            copy.start()

        def send_rows(ch, slot, other):
            q = pltpu.make_async_remote_copy(part(q_hbm, ch), q_all.at[slot, ch], q_send.at[slot, ch], q_recv.at[slot, ch], device_id={'cp': other}, device_id_type=MESH)
            g = pltpu.make_async_remote_copy(part(g_hbm, ch), g_all.at[slot, ch], g_send.at[slot, ch], g_recv.at[slot, ch], device_id={'cp': other}, device_id_type=MESH)
            return q, g

        def send_stat(src_slot, dst_slot, other):
            return pltpu.make_async_remote_copy(stat_pack.at[src_slot], stat_pack.at[dst_slot], stat_send.at[dst_slot], stat_recv.at[dst_slot], device_id={'cp': other}, device_id_type=MESH)

        def forward_rows(ch):
            q = pltpu.make_async_remote_copy(q_all.at[ACROSS, ch], q_all.at[DIAG, ch], q_send.at[DIAG, ch], q_recv.at[DIAG, ch], device_id={'cp': peer}, device_id_type=MESH)
            g = pltpu.make_async_remote_copy(g_all.at[ACROSS, ch], g_all.at[DIAG, ch], g_send.at[DIAG, ch], g_recv.at[DIAG, ch], device_id={'cp': peer}, device_id_type=MESH)
            return q, g

        def send_own_part(ch):
            return pltpu.make_async_remote_copy(dq_all.at[PEER, ch], from_peer_own.at[ch], part_send.at[0, ch], part_recv.at[0, ch], device_id={'cp': peer}, device_id_type=MESH)

        def send_diag_part(ch):
            return pltpu.make_async_remote_copy(dq_all.at[DIAG, ch], from_peer_across.at[ch], part_send.at[1, ch], part_recv.at[1, ch], device_id={'cp': peer}, device_id_type=MESH)

        def send_reduced(ch):
            return pltpu.make_async_remote_copy(dq_all.at[ACROSS, ch], from_across.at[ch], part_send.at[2, ch], part_recv.at[2, ch], device_id={'cp': across}, device_id_type=MESH)

        def unpack_stats(slot):
            both = stat_pack[slot].reshape(unit, 128)
            stat_all[slot, pl.ds(0, group)] = both.reshape(group, rows8, 128)
            stat_all[slot, pl.ds(group, group)] = pltpu.roll(both, 128 - 2 * n_slices, 1).reshape(group, rows8, 128)

        pl.semaphore_wait(barrier, 2)

        def start_rows(ch, slot, other):
            for copy in send_rows(ch, slot, other):
                copy.start()

        start_rows(0, ACROSS, across)
        start_rows(0, PEER, peer)

        for copy in loads[:9]:
            copy.wait()
        lane = lax.broadcasted_iota(jnp.int32, (unit, 128), 1)
        lse_wide[...] = jnp.zeros_like(lse_wide)
        lse_wide[:, :, pl.ds(0, n_slices)] = lse_own[...] * LOG2E
        stats = []
        for kv in range(2):
            acc = jnp.zeros((unit, 128), jnp.float32)
            for s in range(n_slices):
                ch = kv * 2 + s // half_slices
                prod = g_all[OWN, ch, s % half_slices].astype(jnp.float32) * o_own[ch, s % half_slices].astype(jnp.float32)
                acc = jnp.where(lane == 2 * n_slices * kv + n_slices + s, jnp.sum(prod, axis=1, keepdims=True), acc)
            lse = lse_wide[pl.ds(kv * group, group)].reshape(unit, 128)
            stats.append(jnp.where(lane % (2 * n_slices) < n_slices, pltpu.roll(lse, 2 * n_slices, 1) if kv else lse, acc))
        stat_pack[OWN] = jnp.where(lane < 2 * n_slices, stats[0], stats[1]).reshape(group, rows8, 128)
        for slot, other in ((ACROSS, across), (PEER, peer)):
            send_stat(OWN, slot, other).start()
        for ch in range(1, 4):
            for slot, other in ((ACROSS, across), (PEER, peer)):
                start_rows(ch, slot, other)

        unpack_stats(OWN)
        dk_t[...] = jnp.zeros_like(dk_t)
        dv_t[...] = jnp.zeros_like(dv_t)
        token = lax.broadcasted_iota(jnp.int32, (rows8, 128), 0)
        for s in range(half_slices):
            for h in range(group):
                row_pos[pl.ds((s * group + h) * rows8, rows8)] = token + s * slice_len
        for copy in loads[9:]:
            copy.wait()
        for raw, wide, split in ((k_raw, dk_out, k_all), (v_raw, dv_out, v_all)):
            for block in range(n_blocks):
                both = pl.ds(2 * block * KEY_BLOCK, 2 * KEY_BLOCK)
                wide[both] = raw[both].astype(jnp.float32)
                for kv in range(2):
                    split[kv, pl.ds(block * KEY_BLOCK, KEY_BLOCK)] = wide[pl.ds(2 * block * KEY_BLOCK + kv, KEY_BLOCK, stride=2)].astype(jnp.bfloat16)

        def step_body(on_last, step, carry):
            slot = table(step, [a for a, _ in STEPS])
            ch = table(step, [b for _, b in STEPS])
            kv, half = ch // 2, ch % 2
            source = jnp.where(slot == OWN, me, jnp.where(slot == PEER, peer, jnp.where(slot == ACROSS, across, diag)))

            @pl.when(slot != OWN)
            def _():
                pltpu.make_async_remote_copy(q_all.at[slot, ch], q_all.at[slot, ch], q_send.at[slot, ch], q_recv.at[slot, ch], device_id={'cp': peer}, device_id_type=MESH).wait_recv()
                pltpu.make_async_remote_copy(g_all.at[slot, ch], g_all.at[slot, ch], g_send.at[slot, ch], g_recv.at[slot, ch], device_id={'cp': peer}, device_id_type=MESH).wait_recv()

            @pl.when(jnp.logical_and(slot != OWN, ch == 0))
            def _():
                pltpu.make_async_remote_copy(stat_pack.at[slot], stat_pack.at[slot], stat_send.at[slot], stat_recv.at[slot], device_id={'cp': peer}, device_id_type=MESH).wait_recv()
                unpack_stats(slot)

            @pl.when(slot == ACROSS)
            def _():
                for copy in forward_rows(ch):
                    copy.start()

            @pl.when(jnp.logical_and(slot == ACROSS, ch == 0))
            def _():
                send_stat(ACROSS, DIAG, peer).start()

            q_t[...] = q_all[slot, ch].reshape(rows, head_dim).T
            g_t[...] = g_all[slot, ch].reshape(rows, head_dim).T
            for h in range(group):
                st = stat_all[slot, kv * group + h]
                st = jnp.where(half == 1, pltpu.roll(st, 128 - half_slices, 1), st)
                for s in range(half_slices):
                    at = pl.ds((s * group + h) * rows8, rows8)
                    lse_rep[at] = jnp.broadcast_to(st[:, s:s + 1], (rows8, 128))
                    del_rep[at] = jnp.broadcast_to(st[:, n_slices + s:n_slices + s + 1], (rows8, 128))

            def scores(block, p_buf, s_buf, masked):
                keys = pl.ds(block * KEY_BLOCK, KEY_BLOCK)
                logits = dot(q_all[slot, ch].reshape(rows, head_dim), k_all[kv, keys], NT)
                lse = lse_rep[...]
                prob = jnp.exp2(logits * exp_scale - jnp.concatenate([lse, lse], 1))
                if masked:
                    first = me * key_rows + block * KEY_BLOCK - prefix - half * (half_slices * slice_len) - source * rows8
                    key_pos = lax.broadcasted_iota(jnp.int32, (rows, KEY_BLOCK), 1) + first
                    pos = row_pos[...]
                    prob = jnp.where(key_pos <= jnp.concatenate([pos, pos], 1), prob, 0.0)
                grad_prob = dot(g_all[slot, ch].reshape(rows, head_dim), v_all[kv, keys], NT)
                delta = del_rep[...]
                p_buf[...] = prob.astype(jnp.bfloat16)
                s_buf[...] = (prob * (grad_prob - jnp.concatenate([delta, delta], 1))).astype(jnp.bfloat16)

            def grads(block, p_buf, s_buf):
                keys = pl.ds(block * KEY_BLOCK, KEY_BLOCK)
                dv_t[kv, :, keys] += dot(g_t[...], p_buf[...])
                dk_t[kv, :, keys] += dot(q_t[...], s_buf[...])
                part_q = dot(s_buf[...], k_all[kv, keys])
                if block == 0:
                    dq_all[slot, ch] = part_q
                else:
                    dq_all[slot, ch] += part_q

            bufs = ((p_a, s_a), (p_b, s_b))

            masked = [on_last and last * key_rows + (block + 1) * KEY_BLOCK > prefix for block in range(n_blocks)]
            scores(0, *bufs[0], masked[0])
            for block in range(n_blocks):
                if block + 1 < n_blocks:
                    scores(block + 1, *bufs[(block + 1) % 2], masked[block + 1])
                grads(block, *bufs[block % 2])

            @pl.when(slot == PEER)
            def _():
                send_own_part(ch).start()

            @pl.when(slot == DIAG)
            def _():
                send_diag_part(ch).start()

            reduce_ch = jnp.where(
                core == 1,
                table(step, [REDUCE_NEAR.index(i) if i in REDUCE_NEAR else -1 for i in range(len(STEPS))]),
                table(step, [REDUCE_AT.index(i) if i in REDUCE_AT else -1 for i in range(len(STEPS))]))

            @pl.when(reduce_ch >= 0)
            def _():
                send_diag_part(reduce_ch).wait_recv()
                dq_all[ACROSS, reduce_ch] += from_peer_across[reduce_ch]
                send_reduced(reduce_ch).start()

            return carry

        for on_last in (False, True):
            @pl.when((me == last) == on_last)
            def _(on_last=on_last):
                lax.fori_loop(0, len(STEPS), functools.partial(step_body, on_last), 0)

        for acc_t, out, factor in ((dv_t, dv_out, None), (dk_t, dk_out, scale)):
            for block in range(n_blocks):
                for kv in range(2):
                    grad = acc_t[kv, :, pl.ds(block * KEY_BLOCK, KEY_BLOCK)].T
                    out[pl.ds(2 * block * KEY_BLOCK + kv, KEY_BLOCK, stride=2)] = grad if factor is None else grad * factor
        for ch in range(4):
            send_own_part(ch).wait_recv()
            send_reduced(ch).wait_recv()
            total = (dq_all[OWN, ch] + from_peer_own[ch] + from_across[ch]) * scale
            dq_out[pl.ds((ch % 2) * half_slices, half_slices), ch // 2] = total.astype(jnp.bfloat16).reshape(half_slices, unit, head_dim)
        for slot, other in ((ACROSS, across), (PEER, peer)):
            send_stat(OWN, slot, other).wait_send()
            for ch in range(4):
                for copy in send_rows(ch, slot, other):
                    copy.wait_send()
        send_stat(ACROSS, DIAG, peer).wait_send()
        for ch in range(4):
            for copy in forward_rows(ch):
                copy.wait_send()
            send_own_part(ch).wait_send()
            send_diag_part(ch).wait_send()
            send_reduced(ch).wait_send()

    bf16, f32 = jnp.bfloat16, jnp.float32
    chunk = (half_slices, unit, head_dim)
    scratch = [
        pltpu.VMEM((4, 4) + chunk, bf16),
        pltpu.VMEM((4, 4) + chunk, bf16),
        pltpu.VMEM((4, 2 * group, rows8, 128), f32),
        pltpu.VMEM((4, group, rows8, 128), f32),
        pltpu.VMEM((4,) + chunk, bf16),
        pltpu.VMEM((2 * group, rows8, n_slices), f32),
        pltpu.VMEM((2 * group, rows8, 128), f32),
        pltpu.VMEM((2 * key_rows, head_dim), bf16),
        pltpu.VMEM((2 * key_rows, head_dim), bf16),
        pltpu.VMEM((2, key_rows, head_dim), bf16),
        pltpu.VMEM((2, key_rows, head_dim), bf16),
        pltpu.VMEM((2, head_dim, key_rows), f32),
        pltpu.VMEM((2, head_dim, key_rows), f32),
        pltpu.VMEM((4, 4, rows, head_dim), f32),
        pltpu.VMEM((4, rows, head_dim), f32),
        pltpu.VMEM((4, rows, head_dim), f32),
        pltpu.VMEM((4, rows, head_dim), f32),
        pltpu.VMEM((head_dim, rows), bf16),
        pltpu.VMEM((head_dim, rows), bf16),
        pltpu.VMEM((rows, KEY_BLOCK), bf16),
        pltpu.VMEM((rows, KEY_BLOCK), bf16),
        pltpu.VMEM((rows, KEY_BLOCK), bf16),
        pltpu.VMEM((rows, KEY_BLOCK), bf16),
        pltpu.VMEM((rows, 128), f32),
        pltpu.VMEM((rows, 128), f32),
        pltpu.VMEM((rows, 128), jnp.int32),
        pltpu.SemaphoreType.DMA((15,)),
        pltpu.SemaphoreType.DMA((4, 4)),
        pltpu.SemaphoreType.DMA((4, 4)),
        pltpu.SemaphoreType.DMA((4,)),
        pltpu.SemaphoreType.DMA((4, 4)),
        pltpu.SemaphoreType.DMA((4, 4)),
        pltpu.SemaphoreType.DMA((4,)),
        pltpu.SemaphoreType.DMA((3, 4)),
        pltpu.SemaphoreType.DMA((3, 4)),
    ]
    return kernel, scratch


def store_results(dq_in, dk_in, dv_in, dq_hbm, dk_hbm, dv_hbm, sem):
    copies = [pltpu.make_async_copy(a, b, sem.at[i]) for i, (a, b) in enumerate(((dk_in, dk_hbm), (dv_in, dv_hbm), (dq_in, dq_hbm)))]
    for copy in copies:
        copy.start()
    for copy in copies:
        copy.wait()


def solution(mesh):
    cp_size = mesh.shape['cp']
    row_spec = P(None, 'cp', 'tp', None)
    lse_spec = P(None, 'cp', 'tp')
    kv_spec = P('cp', 'tp', None)

    def local_backward(query_in, attn_out, grad_out, log_sum, key_cache, value_cache):
        n_slices, rows8, q_heads, head_dim = query_in.shape
        key_rows, kv_heads, _ = key_cache.shape
        group = q_heads // kv_heads
        kernel, scratch = make_kernel(n_slices, rows8, group, head_dim, key_rows, cp_size)

        def by_head(x):
            return x.transpose(0, 2, 1, 3).reshape(n_slices, kv_heads, group * rows8, head_dim)

        hbm, vmem = pl.BlockSpec(memory_space=pltpu.HBM), pl.BlockSpec(memory_space=pltpu.VMEM)
        grad_q, grad_k, grad_v = pl.pallas_call(
            kernel,
            out_shape=(
                jax.ShapeDtypeStruct((n_slices, kv_heads, group * rows8, head_dim), jnp.bfloat16),
                jax.ShapeDtypeStruct((key_rows * kv_heads, head_dim), jnp.float32),
                jax.ShapeDtypeStruct((key_rows * kv_heads, head_dim), jnp.float32),
            ),
            in_specs=[hbm] * 6,
            out_specs=(vmem,) * 3,
            scratch_shapes=scratch,
            compiler_params=pltpu.CompilerParams(collective_id=0, has_side_effects=True, vmem_limit_bytes=40 * 2 ** 20),
        )(*(pltpu.with_memory_space_constraint(x, pltpu.HBM) for x in (
            by_head(query_in), by_head(attn_out), by_head(grad_out), log_sum.transpose(2, 1, 0),
            key_cache.reshape(key_rows * kv_heads, head_dim), value_cache.reshape(key_rows * kv_heads, head_dim))))
        grad_q, grad_k, grad_v = pl.pallas_call(
            store_results,
            out_shape=tuple(jax.ShapeDtypeStruct(x.shape, x.dtype) for x in (grad_q, grad_k, grad_v)),
            in_specs=[vmem] * 3,
            out_specs=(hbm,) * 3,
            scratch_shapes=[pltpu.SemaphoreType.DMA((3,))],
            compiler_params=pltpu.CompilerParams(vmem_limit_bytes=2 ** 20),
        )(*(pltpu.with_memory_space_constraint(x, pltpu.VMEM) for x in (grad_q, grad_k, grad_v)))
        grad_q = grad_q.reshape(n_slices, q_heads, rows8, head_dim).transpose(0, 2, 1, 3)
        return grad_q, grad_k.reshape(key_rows, kv_heads, head_dim), grad_v.reshape(key_rows, kv_heads, head_dim)

    return jax.shard_map(local_backward, mesh=mesh, in_specs=(row_spec, row_spec, row_spec, lse_spec, kv_spec, kv_spec), out_specs=(row_spec, kv_spec, kv_spec), check_vma=False)
```

```python
import functools

import jax
import jax.numpy as jnp
from jax import lax
from jax.experimental import pallas as pl
from jax.experimental.pallas import tpu as pltpu
from jax.sharding import PartitionSpec as P

MESH = pl.DeviceIdType.MESH
LOG2E = 1.4426950408889634
NT = (((1,), (1,)), ((), ()))
NN = (((1,), (0,)), ((), ()))
KEY_BLOCK = 256
OWN, PEER, ACROSS, DIAG = 0, 1, 2, 3
STEPS = [(0, 0), (1, 0), (0, 1), (2, 0), (3, 0), (2, 1), (3, 1), (1, 1), (2, 2), (3, 2), (2, 3), (3, 3), (0, 2), (1, 2), (0, 3), (1, 3)]
REDUCE_AT = [5, 7, 10, 12]
REDUCE_NEAR = [5, 7, 12, 13]


def dot(a, b, dims=NN):
    return lax.dot_general(a, b, dims, preferred_element_type=jnp.float32)


def table(step, values):
    out = jnp.int32(values[0])
    for i, v in enumerate(values[1:], 1):
        out = jnp.where(step == i, jnp.int32(v), out)
    return out


def make_kernel(n_slices, rows8, group, head_dim, key_rows, cp_size):
    half_slices = n_slices // 2
    unit = rows8 * group
    rows = half_slices * unit
    slice_len = rows8 * cp_size
    prefix = key_rows * cp_size - n_slices * slice_len
    n_blocks = key_rows // KEY_BLOCK
    scale = head_dim ** -0.5
    exp_scale = scale * LOG2E
    last = cp_size - 1
    assert last * key_rows <= prefix

    def kernel(q_hbm, o_hbm, g_hbm, l_hbm, k_hbm, v_hbm, dq_out, dk_out, dv_out,
               q_all, g_all, stat_all, stat_pack, o_own, lse_own, lse_wide, k_raw, v_raw, k_all, v_all, dk_t, dv_t, dq_all,
               from_peer_own, from_peer_across, from_across, q_t, g_t, p_a, s_a, p_b, s_b,
               lse_rep, del_rep, row_pos,
               load_sem, q_recv, g_recv, stat_recv, q_send, g_send, stat_send,
               part_recv, part_send):
        me = lax.axis_index('cp')
        chip, core = me // 2, me % 2
        peer = chip * 2 + (1 - core)
        across = (1 - chip) * 2 + core
        diag = (1 - chip) * 2 + (1 - core)

        barrier = pltpu.get_barrier_semaphore()
        for other in (peer, across):
            pl.semaphore_signal(barrier, inc=1, device_id={'cp': other}, device_id_type=MESH)

        def part(ref, ch):
            return ref.at[pl.ds((ch % 2) * half_slices, half_slices), ch // 2]

        loads = []
        for ch in range(4):
            loads.append(pltpu.make_async_copy(part(g_hbm, ch), g_all.at[OWN, ch], load_sem.at[ch]))
        for ch in range(4):
            loads.append(pltpu.make_async_copy(part(o_hbm, ch), o_own.at[ch], load_sem.at[4 + ch]))
        loads.append(pltpu.make_async_copy(l_hbm, lse_own, load_sem.at[8]))
        for ch in range(4):
            loads.append(pltpu.make_async_copy(part(q_hbm, ch), q_all.at[OWN, ch], load_sem.at[9 + ch]))
        loads.append(pltpu.make_async_copy(k_hbm, k_raw, load_sem.at[13]))
        loads.append(pltpu.make_async_copy(v_hbm, v_raw, load_sem.at[14]))
        for copy in loads:
            copy.start()

        def send_rows(ch, slot, other):
            q = pltpu.make_async_remote_copy(part(q_hbm, ch), q_all.at[slot, ch], q_send.at[slot, ch], q_recv.at[slot, ch], device_id={'cp': other}, device_id_type=MESH)
            g = pltpu.make_async_remote_copy(part(g_hbm, ch), g_all.at[slot, ch], g_send.at[slot, ch], g_recv.at[slot, ch], device_id={'cp': other}, device_id_type=MESH)
            return q, g

        def send_stat(src_slot, dst_slot, other):
            return pltpu.make_async_remote_copy(stat_pack.at[src_slot], stat_pack.at[dst_slot], stat_send.at[dst_slot], stat_recv.at[dst_slot], device_id={'cp': other}, device_id_type=MESH)

        def forward_rows(ch):
            q = pltpu.make_async_remote_copy(q_all.at[ACROSS, ch], q_all.at[DIAG, ch], q_send.at[DIAG, ch], q_recv.at[DIAG, ch], device_id={'cp': peer}, device_id_type=MESH)
            g = pltpu.make_async_remote_copy(g_all.at[ACROSS, ch], g_all.at[DIAG, ch], g_send.at[DIAG, ch], g_recv.at[DIAG, ch], device_id={'cp': peer}, device_id_type=MESH)
            return q, g

        def send_own_part(ch):
            return pltpu.make_async_remote_copy(dq_all.at[PEER, ch], from_peer_own.at[ch], part_send.at[0, ch], part_recv.at[0, ch], device_id={'cp': peer}, device_id_type=MESH)

        def send_diag_part(ch):
            return pltpu.make_async_remote_copy(dq_all.at[DIAG, ch], from_peer_across.at[ch], part_send.at[1, ch], part_recv.at[1, ch], device_id={'cp': peer}, device_id_type=MESH)

        def send_reduced(ch):
            return pltpu.make_async_remote_copy(dq_all.at[ACROSS, ch], from_across.at[ch], part_send.at[2, ch], part_recv.at[2, ch], device_id={'cp': across}, device_id_type=MESH)

        def unpack_stats(slot):
            both = stat_pack[slot].reshape(unit, 128)
            stat_all[slot, pl.ds(0, group)] = both.reshape(group, rows8, 128)
            stat_all[slot, pl.ds(group, group)] = pltpu.roll(both, 128 - 2 * n_slices, 1).reshape(group, rows8, 128)

        pl.semaphore_wait(barrier, 2)

        def start_rows(ch, slot, other):
            for copy in send_rows(ch, slot, other):
                copy.start()

        start_rows(0, ACROSS, across)
        start_rows(0, PEER, peer)

        for copy in loads[:9]:
            copy.wait()
        lane = lax.broadcasted_iota(jnp.int32, (unit, 128), 1)
        lse_wide[...] = jnp.zeros_like(lse_wide)
        lse_wide[:, :, pl.ds(0, n_slices)] = lse_own[...] * LOG2E
        stats = []
        for kv in range(2):
            acc = jnp.zeros((unit, 128), jnp.float32)
            for s in range(n_slices):
                ch = kv * 2 + s // half_slices
                prod = g_all[OWN, ch, s % half_slices].astype(jnp.float32) * o_own[ch, s % half_slices].astype(jnp.float32)
                acc = jnp.where(lane == 2 * n_slices * kv + n_slices + s, jnp.sum(prod, axis=1, keepdims=True), acc)
            lse = lse_wide[pl.ds(kv * group, group)].reshape(unit, 128)
            stats.append(jnp.where(lane % (2 * n_slices) < n_slices, pltpu.roll(lse, 2 * n_slices, 1) if kv else lse, acc))
        stat_pack[OWN] = jnp.where(lane < 2 * n_slices, stats[0], stats[1]).reshape(group, rows8, 128)
        for slot, other in ((ACROSS, across), (PEER, peer)):
            send_stat(OWN, slot, other).start()
        for ch in range(1, 4):
            for slot, other in ((ACROSS, across), (PEER, peer)):
                start_rows(ch, slot, other)

        unpack_stats(OWN)
        dk_t[...] = jnp.zeros_like(dk_t)
        dv_t[...] = jnp.zeros_like(dv_t)
        token = lax.broadcasted_iota(jnp.int32, (rows8, 128), 0)
        for s in range(half_slices):
            for h in range(group):
                row_pos[pl.ds((s * group + h) * rows8, rows8)] = token + s * slice_len
        for copy in loads[9:]:
            copy.wait()
        for raw, wide, split in ((k_raw, dk_out, k_all), (v_raw, dv_out, v_all)):
            for block in range(n_blocks):
                both = pl.ds(2 * block * KEY_BLOCK, 2 * KEY_BLOCK)
                wide[both] = raw[both].astype(jnp.float32)
                for kv in range(2):
                    split[kv, pl.ds(block * KEY_BLOCK, KEY_BLOCK)] = wide[pl.ds(2 * block * KEY_BLOCK + kv, KEY_BLOCK, stride=2)].astype(jnp.bfloat16)

        def step_body(on_last, step, carry):
            slot = table(step, [a for a, _ in STEPS])
            ch = table(step, [b for _, b in STEPS])
            kv, half = ch // 2, ch % 2
            source = jnp.where(slot == OWN, me, jnp.where(slot == PEER, peer, jnp.where(slot == ACROSS, across, diag)))

            @pl.when(slot != OWN)
            def _():
                pltpu.make_async_remote_copy(q_all.at[slot, ch], q_all.at[slot, ch], q_send.at[slot, ch], q_recv.at[slot, ch], device_id={'cp': peer}, device_id_type=MESH).wait_recv()
                pltpu.make_async_remote_copy(g_all.at[slot, ch], g_all.at[slot, ch], g_send.at[slot, ch], g_recv.at[slot, ch], device_id={'cp': peer}, device_id_type=MESH).wait_recv()

            @pl.when(jnp.logical_and(slot != OWN, ch == 0))
            def _():
                pltpu.make_async_remote_copy(stat_pack.at[slot], stat_pack.at[slot], stat_send.at[slot], stat_recv.at[slot], device_id={'cp': peer}, device_id_type=MESH).wait_recv()
                unpack_stats(slot)

            @pl.when(slot == ACROSS)
            def _():
                for copy in forward_rows(ch):
                    copy.start()

            @pl.when(jnp.logical_and(slot == ACROSS, ch == 0))
            def _():
                send_stat(ACROSS, DIAG, peer).start()

            q_t[...] = q_all[slot, ch].reshape(rows, head_dim).T
            g_t[...] = g_all[slot, ch].reshape(rows, head_dim).T
            for h in range(group):
                st = stat_all[slot, kv * group + h]
                st = jnp.where(half == 1, pltpu.roll(st, 128 - half_slices, 1), st)
                for s in range(half_slices):
                    at = pl.ds((s * group + h) * rows8, rows8)
                    lse_rep[at] = jnp.broadcast_to(st[:, s:s + 1], (rows8, 128))
                    del_rep[at] = jnp.broadcast_to(st[:, n_slices + s:n_slices + s + 1], (rows8, 128))

            def scores(block, p_buf, s_buf, masked):
                keys = pl.ds(block * KEY_BLOCK, KEY_BLOCK)
                logits = dot(q_all[slot, ch].reshape(rows, head_dim), k_all[kv, keys], NT)
                lse = lse_rep[...]
                prob = jnp.exp2(logits * exp_scale - jnp.concatenate([lse, lse], 1))
                if masked:
                    first = me * key_rows + block * KEY_BLOCK - prefix - half * (half_slices * slice_len) - source * rows8
                    key_pos = lax.broadcasted_iota(jnp.int32, (rows, KEY_BLOCK), 1) + first
                    pos = row_pos[...]
                    prob = jnp.where(key_pos <= jnp.concatenate([pos, pos], 1), prob, 0.0)
                grad_prob = dot(g_all[slot, ch].reshape(rows, head_dim), v_all[kv, keys], NT)
                delta = del_rep[...]
                p_buf[...] = prob.astype(jnp.bfloat16)
                s_buf[...] = (prob * (grad_prob - jnp.concatenate([delta, delta], 1))).astype(jnp.bfloat16)

            def grads(block, p_buf, s_buf):
                keys = pl.ds(block * KEY_BLOCK, KEY_BLOCK)
                dv_t[kv, :, keys] += dot(g_t[...], p_buf[...])
                dk_t[kv, :, keys] += dot(q_t[...], s_buf[...])
                part_q = dot(s_buf[...], k_all[kv, keys])
                if block == 0:
                    dq_all[slot, ch] = part_q
                else:
                    dq_all[slot, ch] += part_q

            bufs = ((p_a, s_a), (p_b, s_b))

            masked = [on_last and last * key_rows + (block + 1) * KEY_BLOCK > prefix for block in range(n_blocks)]
            scores(0, *bufs[0], masked[0])
            for block in range(n_blocks):
                if block + 1 < n_blocks:
                    scores(block + 1, *bufs[(block + 1) % 2], masked[block + 1])
                grads(block, *bufs[block % 2])

            @pl.when(slot == PEER)
            def _():
                send_own_part(ch).start()

            @pl.when(slot == DIAG)
            def _():
                send_diag_part(ch).start()

            reduce_ch = jnp.where(
                core == 1,
                table(step, [REDUCE_NEAR.index(i) if i in REDUCE_NEAR else -1 for i in range(len(STEPS))]),
                table(step, [REDUCE_AT.index(i) if i in REDUCE_AT else -1 for i in range(len(STEPS))]))

            @pl.when(reduce_ch >= 0)
            def _():
                send_diag_part(reduce_ch).wait_recv()
                dq_all[ACROSS, reduce_ch] += from_peer_across[reduce_ch]
                send_reduced(reduce_ch).start()

            return carry

        for on_last in (False, True):
            @pl.when((me == last) == on_last)
            def _(on_last=on_last):
                lax.fori_loop(0, len(STEPS), functools.partial(step_body, on_last), 0)

        for acc_t, out, factor in ((dv_t, dv_out, None), (dk_t, dk_out, scale)):
            for block in range(n_blocks):
                for kv in range(2):
                    grad = acc_t[kv, :, pl.ds(block * KEY_BLOCK, KEY_BLOCK)].T
                    out[pl.ds(2 * block * KEY_BLOCK + kv, KEY_BLOCK, stride=2)] = grad if factor is None else grad * factor
        for ch in range(4):
            send_own_part(ch).wait_recv()
            send_reduced(ch).wait_recv()
            total = (dq_all[OWN, ch] + from_peer_own[ch] + from_across[ch]) * scale
            dq_out[pl.ds((ch % 2) * half_slices, half_slices), ch // 2] = total.astype(jnp.bfloat16).reshape(half_slices, unit, head_dim)
        for slot, other in ((ACROSS, across), (PEER, peer)):
            send_stat(OWN, slot, other).wait_send()
            for ch in range(4):
                for copy in send_rows(ch, slot, other):
                    copy.wait_send()
        send_stat(ACROSS, DIAG, peer).wait_send()
        for ch in range(4):
            for copy in forward_rows(ch):
                copy.wait_send()
            send_own_part(ch).wait_send()
            send_diag_part(ch).wait_send()
            send_reduced(ch).wait_send()

    bf16, f32 = jnp.bfloat16, jnp.float32
    chunk = (half_slices, unit, head_dim)
    scratch = [
        pltpu.VMEM((4, 4) + chunk, bf16),
        pltpu.VMEM((4, 4) + chunk, bf16),
        pltpu.VMEM((4, 2 * group, rows8, 128), f32),
        pltpu.VMEM((4, group, rows8, 128), f32),
        pltpu.VMEM((4,) + chunk, bf16),
        pltpu.VMEM((2 * group, rows8, n_slices), f32),
        pltpu.VMEM((2 * group, rows8, 128), f32),
        pltpu.VMEM((2 * key_rows, head_dim), bf16),
        pltpu.VMEM((2 * key_rows, head_dim), bf16),
        pltpu.VMEM((2, key_rows, head_dim), bf16),
        pltpu.VMEM((2, key_rows, head_dim), bf16),
        pltpu.VMEM((2, head_dim, key_rows), f32),
        pltpu.VMEM((2, head_dim, key_rows), f32),
        pltpu.VMEM((4, 4, rows, head_dim), f32),
        pltpu.VMEM((4, rows, head_dim), f32),
        pltpu.VMEM((4, rows, head_dim), f32),
        pltpu.VMEM((4, rows, head_dim), f32),
        pltpu.VMEM((head_dim, rows), bf16),
        pltpu.VMEM((head_dim, rows), bf16),
        pltpu.VMEM((rows, KEY_BLOCK), bf16),
        pltpu.VMEM((rows, KEY_BLOCK), bf16),
        pltpu.VMEM((rows, KEY_BLOCK), bf16),
        pltpu.VMEM((rows, KEY_BLOCK), bf16),
        pltpu.VMEM((rows, 128), f32),
        pltpu.VMEM((rows, 128), f32),
        pltpu.VMEM((rows, 128), jnp.int32),
        pltpu.SemaphoreType.DMA((15,)),
        pltpu.SemaphoreType.DMA((4, 4)),
        pltpu.SemaphoreType.DMA((4, 4)),
        pltpu.SemaphoreType.DMA((4,)),
        pltpu.SemaphoreType.DMA((4, 4)),
        pltpu.SemaphoreType.DMA((4, 4)),
        pltpu.SemaphoreType.DMA((4,)),
        pltpu.SemaphoreType.DMA((3, 4)),
        pltpu.SemaphoreType.DMA((3, 4)),
    ]
    return kernel, scratch


def store_results(dq_in, dk_in, dv_in, dq_hbm, dk_hbm, dv_hbm, sem):
    copies = [pltpu.make_async_copy(a, b, sem.at[i]) for i, (a, b) in enumerate(((dk_in, dk_hbm), (dv_in, dv_hbm), (dq_in, dq_hbm)))]
    for copy in copies:
        copy.start()
    for copy in copies:
        copy.wait()


def solution(mesh):
    cp_size = mesh.shape['cp']
    row_spec = P(None, 'cp', 'tp', None)
    lse_spec = P(None, 'cp', 'tp')
    kv_spec = P('cp', 'tp', None)

    def local_backward(query_in, attn_out, grad_out, log_sum, key_cache, value_cache):
        n_slices, rows8, q_heads, head_dim = query_in.shape
        key_rows, kv_heads, _ = key_cache.shape
        group = q_heads // kv_heads
        kernel, scratch = make_kernel(n_slices, rows8, group, head_dim, key_rows, cp_size)

        def by_head(x):
            return x.transpose(0, 2, 1, 3).reshape(n_slices, kv_heads, group * rows8, head_dim)

        hbm, vmem = pl.BlockSpec(memory_space=pltpu.HBM), pl.BlockSpec(memory_space=pltpu.VMEM)
        grad_q, grad_k, grad_v = pl.pallas_call(
            kernel,
            out_shape=(
                jax.ShapeDtypeStruct((n_slices, kv_heads, group * rows8, head_dim), jnp.bfloat16),
                jax.ShapeDtypeStruct((key_rows * kv_heads, head_dim), jnp.float32),
                jax.ShapeDtypeStruct((key_rows * kv_heads, head_dim), jnp.float32),
            ),
            in_specs=[hbm] * 6,
            out_specs=(vmem,) * 3,
            scratch_shapes=scratch,
            compiler_params=pltpu.CompilerParams(collective_id=0, has_side_effects=True, vmem_limit_bytes=40 * 2 ** 20),
        )(*(pltpu.with_memory_space_constraint(x, pltpu.HBM) for x in (
            by_head(query_in), by_head(attn_out), by_head(grad_out), log_sum.transpose(2, 1, 0),
            key_cache.reshape(key_rows * kv_heads, head_dim), value_cache.reshape(key_rows * kv_heads, head_dim))))
        grad_q, grad_k, grad_v = pl.pallas_call(
            store_results,
            out_shape=tuple(jax.ShapeDtypeStruct(x.shape, x.dtype) for x in (grad_q, grad_k, grad_v)),
            in_specs=[vmem] * 3,
            out_specs=(hbm,) * 3,
            scratch_shapes=[pltpu.SemaphoreType.DMA((3,))],
            compiler_params=pltpu.CompilerParams(vmem_limit_bytes=2 ** 20),
        )(*(pltpu.with_memory_space_constraint(x, pltpu.VMEM) for x in (grad_q, grad_k, grad_v)))
        grad_q = grad_q.reshape(n_slices, q_heads, rows8, head_dim).transpose(0, 2, 1, 3)
        return grad_q, grad_k.reshape(key_rows, kv_heads, head_dim), grad_v.reshape(key_rows, kv_heads, head_dim)

    return jax.shard_map(local_backward, mesh=mesh, in_specs=(row_spec, row_spec, row_spec, lse_spec, kv_spec, kv_spec), out_specs=(row_spec, kv_spec, kv_spec), check_vma=False)
```
